128 devices in a mesh: grp: 8 (over y, core), inner: 16 (over z, x).
Axes of the slice: x: 4, y: 4, z: 4, core: 2. Of those that a mesh axis runs over, the one named last changes fastest.
Arguments:
- grad_out: bfloat16 [16384, 2048], P(('grp', 'inner')), may hold values from -6 to 6
- hidden: bfloat16 [16384, 2048], P(('grp', 'inner')), may hold values from -6 to 6
- norm_gain: float32 [2048], replicated, may hold values from 0.25 to 1.75
- expert_ids: int32 [16384, 8], P(('grp', 'inner')), may hold values from 0 to 127, all different within a row; in each aligned block of 128 rows (0 to 127, 128 to 255, ...) at most 10 rows name the same one
- gate_weights: float32 [16384, 8], P(('grp', 'inner')), may hold values from 0.02 to 0.5
- w_gate: bfloat16 [128, 2048, 768], P(('grp', 'inner')), may hold values from -0.125 to 0.125
- w_up: bfloat16 [128, 2048, 768], P(('grp', 'inner')), may hold values from -0.125 to 0.125
- w_down: bfloat16 [128, 768, 2048], P(('grp', 'inner')), may hold values from -0.21875 to 0.21875
- w_out: bfloat16 [4096, 2048], P('inner'), may hold values from -0.09375 to 0.09375
- queries: bfloat16 [16384, 4096], P(('grp', 'inner')), may hold values from -0.6 to 0.6
- keys: bfloat16 [16384, 512], P(('grp', 'inner')), may hold values from -0.6 to 0.6
- values: bfloat16 [16384, 512], P(('grp', 'inner')), may hold values from -6 to 6
- attn_out: bfloat16 [16384, 4096], P(('grp', 'inner')), may hold values from -6 to 6
- lse: float32 [32, 16384], P('inner', 'grp'), as said below
Outputs:
- grad_resid: bfloat16 [16384, 2048], P(('grp', 'inner'))
- queries_gradient: bfloat16 [16384, 4096], P(('grp', 'inner'))
- keys_gradient: bfloat16 [16384, 512], P(('grp', 'inner'))
- values_gradient: bfloat16 [16384, 512], P(('grp', 'inner'))
The draws below stay inside these ranges and needn't reach their ends.
Inputs may be any that keep to these rules, and one draw needn't show every extreme that they name: `expert_ids`: each token names 8 different experts. Among the 128 tokens of one device (aligned blocks of rows), no expert is named by more than 10 tokens; in some device's tokens one expert is named by exactly 10. lse[h, t] minus log(1 + the position of token t in its sequence of 2048) lies between 0 and 1.5.
All inputs are finite; a program needn't handle non-finite values.
Results may differ from the reference program's by a relative error of at most 0.012.
Values may be sent and summed in bfloat16 or wider, within the bound.
No kernel may reach another device: no remote copies, remote signals or barrier semaphores. Data moves between devices by JAX's collectives and lax.ppermute only.
A program may use at most 192 MiB of HBM per device.

```python
import math
import jax
import jax.numpy as jnp
import numpy as np
from jax import lax

D = 2048
QUERY_HEADS = 32
KEY_VALUE_HEADS = 4
HEAD_SIZE = 128
FF = 768
TOPK = 8
TOK_DEV = 128
EXPERTS = 128
CAP = 10
SEQUENCE_TOKENS = 2048
TOTAL_TOKENS = 16384


def draw_lse(key, part):
    position = (jnp.arange(TOTAL_TOKENS, dtype=jnp.int32) % SEQUENCE_TOKENS).astype(jnp.float32)
    base = jnp.log(position + 1.0)[None, :]
    extra = jax.random.uniform(key, (QUERY_HEADS, TOTAL_TOKENS), jnp.float32, 0.3, 1.2)
    return base + extra


def bounded_rows(key, columns):
    second = jax.random.fold_in(key, 23)
    drawn = jax.random.uniform(second, (TOTAL_TOKENS, columns), jnp.float32, -0.59, 0.59)
    return drawn.astype(jnp.bfloat16)


def draw_queries(key, part):
    return bounded_rows(jax.random.fold_in(key, 101), QUERY_HEADS * HEAD_SIZE)


def draw_keys(key, part):
    return bounded_rows(jax.random.fold_in(key, 202), KEY_VALUE_HEADS * HEAD_SIZE)


def shard_levels(own_key, shape, pieces, least, top_value):
    def one(dim, blocks):
        draws = jax.random.uniform(jax.random.fold_in(jax.random.fold_in(own_key, 6), dim), (blocks,), jnp.float32, least / len(pieces), top_value / len(pieces))
        return jnp.repeat(jnp.exp(draws), shape[dim] // blocks).reshape((-1,) + (1,) * (len(shape) - dim - 1))

    factor_of = one(*pieces[0])
    for cut in pieces[1:]:
        factor_of = factor_of * one(*cut)
    return factor_of


def shared_out(rng, own, number, rows, count, top, most, skew):
    order = jax.random.permutation(rng, count)
    crowded, usual = load_shares(count, rows * top, most, skew, True), load_shares(count, rows * top, most, skew, False)
    places = jnp.arange(count)

    def named(tallies, turn):
        used = int((tallies > 0).sum())
        fixed = max(1, used // 4)
        moved = fixed + (places - fixed + turn * (used - fixed)) % max(1, count - fixed)
        return jnp.zeros((count,), jnp.int32).at[order[jnp.where(places < fixed, places, moved)]].set(jnp.asarray(tallies, jnp.int32))

    tallies = jnp.where(number % 4 == 0, named(crowded, number // 4), named(usual, number - number // 4 - 1))
    mixed = jax.random.permutation(jax.random.fold_in(own, 3), count)
    giver, receiver = mixed[0:count // 2 * 2:2], mixed[1:count // 2 * 2:2]
    slack = jnp.minimum(tallies[giver] - 1, most - tallies[receiver]) // 2
    slack = jnp.where((giver == order[0]) | (receiver == order[0]) | (tallies[receiver] == 0), 0, jnp.maximum(slack, 0))
    moved = jax.random.randint(jax.random.fold_in(own, 4), (count // 2,), 0, 1 << 20) % (slack + 1)
    tallies = tallies.at[giver].add(-moved).at[receiver].add(moved)
    members = jnp.searchsorted(jnp.cumsum(tallies), jnp.arange(rows * top), side="right").astype(jnp.int32)
    grid = members.reshape(top, rows).T
    grid = grid[jax.random.permutation(jax.random.fold_in(own, 1), rows)]
    turn = jax.random.randint(jax.random.fold_in(own, 2), (rows, 1), 0, top)
    return jnp.take_along_axis(grid, (jnp.arange(top)[None, :] + turn) % top, axis=1)


def load_shares(count, total, reach, slope, full):
    loads = [(1 << 20) // math.isqrt(grade ** slope) + 1 for grade in range(1, count + 1)]
    largest = reach if full else min(reach, max(-(-total // count), total * loads[0] // sum(loads)))
    least = 1 if total - largest >= count - 1 else 0
    given, surplus = [largest] + [least] * (count - 1), total - largest - least * (count - 1)
    while surplus > 0:
        movable = [i for i in range(1, count) if given[i] < largest] or [i for i in range(1, count) if given[i] < reach]
        pool, left = sum([loads[i] for i in movable]), surplus
        for i in movable:
            more = min(reach - given[i], max(1, left * loads[i] // pool), surplus)
            given[i] = given[i] + more
            surplus = surplus - more
    return np.array(given)


def normal_values(key, extent, width, bound, pieces=(), kind=jnp.bfloat16):
    values = jax.random.normal(key, extent, jnp.float32) * width
    if len(pieces) > 0:
        values = shard_levels(key, extent, pieces, -0.22, 0.18) * values
    return jnp.clip(values, min=-bound, max=bound).astype(kind)


def setup_inputs(seed: int = 0) -> dict:
    splits = jax.random.split(jax.random.key(seed), 15)
    grad_out = normal_values(splits[0], (TOTAL_TOKENS, D), 1.0, 6.0, ((0, 128),))
    hidden = normal_values(splits[1], (TOTAL_TOKENS, D), 1.0, 6.0, ((0, 128),))
    norm_gain = jnp.clip(1.0 + 0.15 * jax.random.normal(splits[2], (D,), jnp.float32), 0.25, 1.75)
    expert_ids_keys = jax.random.split(jax.random.fold_in(splits[3], 1), TOTAL_TOKENS // TOK_DEV)
    expert_ids_turns = jax.random.permutation(jax.random.fold_in(splits[3], 3), TOTAL_TOKENS // TOK_DEV)
    expert_ids = jax.vmap(lambda own, number: shared_out(jax.random.fold_in(splits[3], 2), own, number, TOK_DEV, EXPERTS, TOPK, CAP, 1))(expert_ids_keys, expert_ids_turns).reshape((TOTAL_TOKENS, TOPK))
    gate_weights = jnp.clip(jnp.exp(math.log(0.5) - 3.218876 * jax.random.uniform(splits[4], (TOTAL_TOKENS, TOPK), jnp.float32) ** shard_levels(splits[4], (TOTAL_TOKENS, TOPK), ((0, 128),), -0.2, 0.2)), 0.02, 0.5)
    w_gate = normal_values(splits[5], (EXPERTS, D, FF), D ** -0.5, 0.125, ((0, 128),))
    w_up = normal_values(splits[6], (EXPERTS, D, FF), D ** -0.5, 0.125, ((0, 128),))
    w_down = normal_values(splits[7], (EXPERTS, FF, D), FF ** -0.5, 0.21875, ((0, 128),))
    w_out = normal_values(splits[8], (QUERY_HEADS * HEAD_SIZE, D), (QUERY_HEADS * HEAD_SIZE) ** -0.5, 0.09375, ((0, 16),))
    queries = draw_queries(jax.random.fold_in(splits[14], 71), 0)
    keys = draw_keys(jax.random.fold_in(splits[14], 71), 0)
    values = normal_values(splits[11], (TOTAL_TOKENS, KEY_VALUE_HEADS * HEAD_SIZE), 1.0, 6.0, ((0, 128),))
    attn_out = normal_values(splits[12], (TOTAL_TOKENS, QUERY_HEADS * HEAD_SIZE), 1.0, 6.0, ((0, 128),))
    lse = draw_lse(jax.random.fold_in(splits[14], 71), 0)
    return {"grad_out": grad_out, "hidden": hidden, "norm_gain": norm_gain, "expert_ids": expert_ids, "gate_weights": gate_weights, "w_gate": w_gate, "w_up": w_up, "w_down": w_down, "w_out": w_out, "queries": queries, "keys": keys, "values": values, "attn_out": attn_out, "lse": lse}


def contract_last(left, right):
    return lax.dot_general(left, right, (((1,), (1,)), ((), ())), preferred_element_type=jnp.float32)

def expert_back(inputs, upstream, gate_matrix, up_matrix, down_matrix):
    gate_pre = jnp.dot(inputs, gate_matrix, preferred_element_type=jnp.float32)
    up_pre = jnp.dot(inputs, up_matrix, preferred_element_type=jnp.float32)
    back_hidden = contract_last(upstream, down_matrix)
    sigmoid = jax.nn.sigmoid(gate_pre)
    grad_gate = (back_hidden * up_pre * sigmoid * (1.0 + gate_pre * (1.0 - sigmoid))).astype(jnp.bfloat16)
    grad_up = (back_hidden * gate_pre * sigmoid).astype(jnp.bfloat16)
    grad_in = contract_last(grad_gate, gate_matrix) + contract_last(grad_up, up_matrix)
    return grad_in.astype(jnp.bfloat16)

def head_group(operands):
    query_blk, output_blk, grad_blk, key_blk, value_blk, lse_blk = operands
    scale = float(HEAD_SIZE) ** (-0.5)
    query_f = query_blk.astype(jnp.float32)
    key_f = key_blk.astype(jnp.float32)
    value_f = value_blk.astype(jnp.float32)
    grad_f = grad_blk.astype(jnp.float32)
    output_f = output_blk.astype(jnp.float32)
    scores = jnp.einsum('gid,jd->gij', query_f, key_f) * scale
    position = jnp.arange(SEQUENCE_TOKENS, dtype=jnp.int32)
    visible = position[None, :] <= position[:, None]
    probs = jnp.where(visible[None], jnp.exp(scores - lse_blk[:, :, None]), 0.0)
    probs_low = probs.astype(jnp.bfloat16).astype(jnp.float32)
    grad_probs = jnp.einsum('gid,jd->gij', grad_f, value_f)
    delta = lax.optimization_barrier(jnp.sum(grad_f * output_f, axis=-1))
    grad_scores = (probs * (grad_probs - delta[:, :, None])).astype(jnp.bfloat16).astype(jnp.float32)
    query_gradient_fn = jnp.einsum('gij,jd->gid', grad_scores, key_f) * scale
    key_gradient_fn = jnp.einsum('gij,gid->jd', grad_scores, query_f) * scale
    value_gradient_fn = jnp.einsum('gij,gid->jd', probs_low, grad_f)
    return (query_gradient_fn.astype(jnp.bfloat16), key_gradient_fn.astype(jnp.bfloat16), value_gradient_fn.astype(jnp.bfloat16))

def reference(grad_out, hidden, norm_gain, expert_ids, gate_weights, w_gate, w_up, w_down, w_out, queries, keys, values, attn_out, lse):
    hidden_f = hidden.astype(jnp.float32)
    inverse = lax.rsqrt(lax.optimization_barrier(jnp.mean(hidden_f * hidden_f, axis=1, keepdims=True)) + 1e-06)
    normed = (hidden_f * inverse * norm_gain).astype(jnp.bfloat16)
    upstream = grad_out.astype(jnp.float32)
    flat_count = TOTAL_TOKENS * TOPK
    flat_ids = expert_ids.reshape(-1)
    flat_weights = gate_weights.reshape(-1)
    order = jnp.argsort(flat_ids, stable=True).astype(jnp.int32)
    counts = lax.optimization_barrier(jnp.sum((flat_ids[:, None] == jnp.arange(EXPERTS, dtype=jnp.int32)[None, :]).astype(jnp.int32), axis=0))
    starts = jnp.cumsum(counts) - counts
    most = TOTAL_TOKENS // TOK_DEV * CAP

    def one_expert(total, expert):
        offsets = jnp.arange(most, dtype=jnp.int32)
        place = starts[expert] + offsets
        valid = offsets < counts[expert]
        rows = order[jnp.minimum(place, flat_count - 1)]
        tok_index = rows // TOPK
        inputs = normed[tok_index]
        scaled = (upstream[tok_index] * flat_weights[rows][:, None]).astype(jnp.bfloat16)
        grad_in = expert_back(inputs, scaled, w_gate[expert], w_up[expert], w_down[expert])
        grad_in = jnp.where(valid[:, None], grad_in.astype(jnp.float32), 0.0)
        return (total.at[tok_index].add(grad_in), None)
    grad_normed, _ = lax.scan(one_expert, jnp.zeros((TOTAL_TOKENS, D), jnp.float32), jnp.arange(EXPERTS, dtype=jnp.int32))
    gained = grad_normed * norm_gain
    statistic = lax.optimization_barrier(jnp.mean(gained * hidden_f, axis=1, keepdims=True))
    grad_resid = (upstream + inverse * gained - hidden_f * inverse * inverse * inverse * statistic).astype(jnp.bfloat16)
    grad_attn = contract_last(grad_resid, w_out).astype(jnp.bfloat16)
    sequence_count = TOTAL_TOKENS // SEQUENCE_TOKENS
    shared_result = QUERY_HEADS // KEY_VALUE_HEADS

    def by_head(numeric_array):
        return numeric_array.reshape(sequence_count, SEQUENCE_TOKENS, KEY_VALUE_HEADS, shared_result, HEAD_SIZE).transpose(0, 2, 3, 1, 4).reshape(sequence_count * KEY_VALUE_HEADS, shared_result, SEQUENCE_TOKENS, HEAD_SIZE)

    def by_kv(numeric_array):
        return numeric_array.reshape(sequence_count, SEQUENCE_TOKENS, KEY_VALUE_HEADS, HEAD_SIZE).transpose(0, 2, 1, 3).reshape(sequence_count * KEY_VALUE_HEADS, SEQUENCE_TOKENS, HEAD_SIZE)
    logsumexp_heads = lse.reshape(KEY_VALUE_HEADS, shared_result, sequence_count, SEQUENCE_TOKENS).transpose(2, 0, 1, 3).reshape(sequence_count * KEY_VALUE_HEADS, shared_result, SEQUENCE_TOKENS)
    query_gradient_fn, key_gradient_fn, value_gradient_fn = lax.map(head_group, (by_head(queries), by_head(attn_out), by_head(grad_attn), by_kv(keys), by_kv(values), logsumexp_heads))
    queries_gradient = query_gradient_fn.reshape(sequence_count, KEY_VALUE_HEADS, shared_result, SEQUENCE_TOKENS, HEAD_SIZE).transpose(0, 3, 1, 2, 4).reshape(TOTAL_TOKENS, QUERY_HEADS * HEAD_SIZE)
    keys_gradient = key_gradient_fn.reshape(sequence_count, KEY_VALUE_HEADS, SEQUENCE_TOKENS, HEAD_SIZE).transpose(0, 2, 1, 3).reshape(TOTAL_TOKENS, KEY_VALUE_HEADS * HEAD_SIZE)
    values_gradient = value_gradient_fn.reshape(sequence_count, KEY_VALUE_HEADS, SEQUENCE_TOKENS, HEAD_SIZE).transpose(0, 2, 1, 3).reshape(TOTAL_TOKENS, KEY_VALUE_HEADS * HEAD_SIZE)
    return (grad_resid, queries_gradient, keys_gradient, values_gradient)
```

```python
import functools
import math

import jax
import jax.numpy as jnp
from jax import lax
from jax.experimental import pallas as pl
from jax.experimental.pallas import tpu as pltpu
from jax.sharding import PartitionSpec as P

KEY_VALUE_HEADS = 4
HEAD_SIZE = 128
EPSILON = 1e-06
BLOCK = 512
HALVES = 2
DELTA_ROWS = 16


def dot_nn(left, right):
    return lax.dot_general(
        left, right, (((1,), (0,)), ((), ())), preferred_element_type=jnp.float32
    )


def contract_last(left, right):
    return lax.dot_general(
        left, right, (((1,), (1,)), ((), ())), preferred_element_type=jnp.float32
    )


def contract_first(left, right):
    return lax.dot_general(
        left, right, (((0,), (0,)), ((), ())), preferred_element_type=jnp.float32
    )


def project_kernel(resid_ref, weight_ref, output_ref, out_ref, *, head):
    parts, devices = weight_ref.shape[:2]
    piece = weight_ref.shape[3]
    total = None
    for part in range(parts):
        weight = weight_ref[part].reshape(devices * HEAD_SIZE, piece)
        term = contract_last(weight, resid_ref[:, part * piece : (part + 1) * piece])
        total = term if total is None else total + term
    head_width = output_ref.shape[1] // devices
    row_at = lax.broadcasted_iota(jnp.int32, (DELTA_ROWS, resid_ref.shape[0]), 0)
    for device in range(devices):
        grad = total[device * HEAD_SIZE : (device + 1) * HEAD_SIZE].astype(jnp.bfloat16)
        start = device * head_width + head * HEAD_SIZE
        output = output_ref[:, start : start + HEAD_SIZE].astype(jnp.float32).T
        rest = jnp.sum(grad.astype(jnp.float32) * output, axis=0, keepdims=True)
        held = jnp.zeros(row_at.shape, jnp.float32)
        for row in range(3):
            digit = rest.astype(jnp.bfloat16).astype(jnp.float32)
            held = jnp.where(row_at == row, digit, held)
            rest = rest - digit
        out_ref[device, :HEAD_SIZE] = grad
        out_ref[device, HEAD_SIZE:] = held.astype(jnp.bfloat16)


def project(resid, weights, attn_out, head):
    tokens, width = resid.shape
    parts, devices, heads, _, piece = weights.shape
    step = min(4, devices)
    head_rows = HEAD_SIZE + DELTA_ROWS
    return pl.pallas_call(
        functools.partial(project_kernel, head=head),
        grid=(devices // step,),
        in_specs=[
            pl.BlockSpec((tokens, width), lambda n: (0, 0)),
            pl.BlockSpec(
                (parts, step, None, HEAD_SIZE, piece), lambda n: (0, n, head, 0, 0)
            ),
            pl.BlockSpec((tokens, step * heads * HEAD_SIZE), lambda n: (0, n)),
        ],
        out_specs=pl.BlockSpec((step, head_rows, tokens), lambda n: (n, 0, 0)),
        out_shape=jax.ShapeDtypeStruct((devices, head_rows, tokens), jnp.bfloat16),
        cost_estimate=pl.CostEstimate(
            flops=2 * tokens * width * devices * HEAD_SIZE,
            bytes_accessed=2 * devices * HEAD_SIZE * (width + 3 * tokens),
            transcendentals=0,
        ),
    )(resid, weights, attn_out)


def attention_kernel(packed_ref, grad_ref, lse_ref, *refs, head, heads):
    last = head == heads - 1
    before_ref = refs[0] if head > 0 else None
    if last:
        out_ref, delta_ref, grad_t_ref, dqt_ref = refs[-4:]
    else:
        dquery_ref, dkv_ref, delta_ref, grad_t_ref, dqt_ref = refs[-5:]
    j = pl.program_id(0)
    steps = pl.num_programs(0)
    length = packed_ref.shape[0]
    devices, _, tokens = grad_ref.shape
    block = min(BLOCK, length)
    scale = float(HEAD_SIZE) ** (-0.5)
    log2e = math.log2(math.e)
    key_from = heads * HEAD_SIZE
    value_from = key_from + HEAD_SIZE
    query_cols = slice(head * HEAD_SIZE, (head + 1) * HEAD_SIZE)

    @pl.when(j == 0)
    def _():
        dqt_ref[...] = jnp.zeros_like(dqt_ref)
        for device in range(devices):
            cols = slice(device * tokens, (device + 1) * tokens)
            grad_t_ref[:, cols] = grad_ref[device, :HEAD_SIZE]
            digits = grad_ref[device, HEAD_SIZE:].astype(jnp.float32)
            delta_ref[:, cols] = jnp.broadcast_to(
                jnp.sum(digits, axis=0, keepdims=True), (8, tokens)
            )

    key_rows = pl.ds(pl.multiple_of(j * block, block), block)
    key = packed_ref[key_rows, key_from:value_from]
    value = packed_ref[key_rows, value_from : value_from + HEAD_SIZE]
    key_t = key.astype(jnp.float32).T.astype(jnp.bfloat16)

    def one(i, masked):
        rows = pl.ds(pl.multiple_of(i * block, block), block)
        query = packed_ref[rows, query_cols]
        grad_t = grad_t_ref[:, rows]
        lse = lse_ref[head : head + 1, rows] * log2e
        delta = delta_ref[0:1, rows]
        scores = contract_last(key, query)
        probs = jnp.exp2(scores * (scale * log2e) - lse)
        if masked:
            key_at = lax.broadcasted_iota(jnp.int32, scores.shape, 0)
            query_at = lax.broadcasted_iota(jnp.int32, scores.shape, 1)
            probs = jnp.where(key_at <= query_at, probs, 0.0)
        grad_probs = dot_nn(value, grad_t)
        grad_scores = (probs * (grad_probs - delta)).astype(jnp.bfloat16)
        dkey = dot_nn(grad_scores, query)
        dvalue = contract_last(probs.astype(jnp.bfloat16), grad_t)
        dqt_ref[:, rows] += dot_nn(key_t, grad_scores)
        return dkey, dvalue

    def body(i, carry):
        dkey, dvalue = one(i, False)
        return carry[0] + dkey, carry[1] + dvalue

    dkey, dvalue = lax.fori_loop(j + 1, steps, body, one(j, True))
    dkey = dkey * scale
    if before_ref is not None:
        dkey = dkey + before_ref[key_rows, :HEAD_SIZE]
        dvalue = dvalue + before_ref[key_rows, HEAD_SIZE:]
    if last:
        out_ref[key_rows, HEAD_SIZE : 2 * HEAD_SIZE] = dkey.astype(jnp.bfloat16)
        out_ref[key_rows, 2 * HEAD_SIZE :] = dvalue.astype(jnp.bfloat16)
    else:
        dkv_ref[key_rows, :HEAD_SIZE] = dkey
        dkv_ref[key_rows, HEAD_SIZE:] = dvalue

    @pl.when(j == steps - 1)
    def _():
        dquery = (dqt_ref[...].T * scale).astype(jnp.bfloat16)
        if last:
            out_ref[:, :HEAD_SIZE] = dquery
        else:
            dquery_ref[...] = dquery


def attention(packed, grad, lse, head, before):
    length, packed_width = packed.shape
    heads = lse.shape[0]
    last = head == heads - 1
    block = min(BLOCK, length)
    operands = [packed, grad, lse] + ([before] if head > 0 else [])

    def whole(shape):
        return pl.BlockSpec(shape, lambda j: (0,) * len(shape))

    if last:
        shapes = [jax.ShapeDtypeStruct((length, 3 * HEAD_SIZE), jnp.bfloat16)]
    else:
        shapes = [
            jax.ShapeDtypeStruct((length, HEAD_SIZE), jnp.bfloat16),
            jax.ShapeDtypeStruct((length, 2 * HEAD_SIZE), jnp.float32),
        ]
    return pl.pallas_call(
        functools.partial(attention_kernel, head=head, heads=heads),
        grid=(length // block,),
        in_specs=[whole(operand.shape) for operand in operands],
        out_specs=[whole(shape.shape) for shape in shapes],
        out_shape=shapes,
        scratch_shapes=[
            pltpu.VMEM((8, length), jnp.float32),
            pltpu.VMEM((HEAD_SIZE, length), jnp.bfloat16),
            pltpu.VMEM((HEAD_SIZE, length), jnp.float32),
        ],
        compiler_params=pltpu.CompilerParams(
            dimension_semantics=("arbitrary",), vmem_limit_bytes=48 * 1024 * 1024
        ),
        cost_estimate=pl.CostEstimate(
            flops=10 * length * length * HEAD_SIZE // 2,
            bytes_accessed=2 * length * (packed_width + 6 * HEAD_SIZE),
            transcendentals=length * length // 2,
        ),
    )(*operands)


def per_device(
    grad_out,
    hidden,
    norm_gain,
    expert_ids,
    gate_weights,
    w_gate,
    w_up,
    w_down,
    w_out,
    queries,
    keys,
    values,
    attn_out,
    lse,
):
    bf16, f32 = jnp.bfloat16, jnp.float32
    rows, width = hidden.shape
    topk = expert_ids.shape[1]
    groups = lax.axis_size("grp")
    inner = lax.axis_size("inner")
    grp_at = lax.axis_index("grp")
    experts = groups * inner
    capacity = max(2, 5 * rows * topk // (4 * experts))
    slots = groups * capacity
    column = groups * rows
    ff = w_gate.shape[2]
    head_width = queries.shape[1] // inner
    shared = inner // KEY_VALUE_HEADS

    hidden_f = hidden.astype(f32)
    inverse = lax.rsqrt(jnp.mean(hidden_f * hidden_f, axis=1, keepdims=True) + EPSILON)
    normed = (hidden_f * inverse * norm_gain).astype(bf16)

    normed_all = lax.all_gather(normed, "grp", axis=0, tiled=True)
    upstream_all = lax.all_gather(grad_out, "grp", axis=0, tiled=True)
    routing = jnp.concatenate([expert_ids.astype(f32).T, gate_weights.T], axis=0)
    routing = lax.all_gather(routing, "grp", axis=0, tiled=False)

    piece = width // groups
    w_piece = lax.dynamic_slice_in_dim(w_out, grp_at * piece, piece, axis=1)
    w_piece = lax.all_to_all(
        jnp.broadcast_to(w_piece[None], (inner,) + w_piece.shape), "inner", 0, 0, tiled=True
    )
    normed_all, w_piece = lax.optimization_barrier((normed_all, w_piece))
    w_whole = lax.all_gather(w_piece, "grp", axis=0, tiled=False)
    w_whole = w_whole.reshape(groups, inner, head_width // HEAD_SIZE, HEAD_SIZE, piece)

    kv = jnp.stack(
        [
            keys.reshape(rows, KEY_VALUE_HEADS, HEAD_SIZE),
            values.reshape(rows, KEY_VALUE_HEADS, HEAD_SIZE),
        ],
        axis=2,
    ).reshape(rows, KEY_VALUE_HEADS, 2 * HEAD_SIZE)
    kv = jnp.repeat(kv.transpose(1, 0, 2), shared, axis=0)
    packed = jnp.concatenate(
        [queries.reshape(rows, inner, head_width).transpose(1, 0, 2), kv], axis=2
    )

    ids_all = routing[:, :topk]
    gates_all = routing[:, topk:]
    mine = (grp_at * inner + lax.broadcasted_iota(jnp.int32, (1, inner, 1, 1), 1)).astype(f32)
    match = ids_all[:, None] == mine
    named = jnp.any(match, axis=2)
    gate = jnp.sum(jnp.where(match, gates_all[:, None], 0.0), axis=2)
    before = (
        lax.broadcasted_iota(jnp.int32, (rows, rows), 0)
        < lax.broadcasted_iota(jnp.int32, (rows, rows), 1)
    ).astype(bf16)
    rank = dot_nn(named.astype(bf16).reshape(groups * inner, rows), before)
    rank = rank.reshape(groups, inner, rows)
    block_at = lax.broadcasted_iota(jnp.int32, (groups, 1, 1), 0).astype(f32)
    slot = jnp.where(named, block_at * capacity + rank, -1.0)
    slot = slot.transpose(1, 0, 2).reshape(inner, 1, column)
    gate = gate.transpose(1, 0, 2).reshape(inner, 1, column)
    slot_at = lax.broadcasted_iota(jnp.int32, (1, slots, 1), 1).astype(f32)
    chosen = slot == slot_at
    picks = chosen.astype(bf16).reshape(inner * slots, column)
    slot_gate = jnp.sum(jnp.where(chosen, gate, 0.0), axis=2).reshape(inner * slots, 1)

    def to_experts(array):
        array = array.astype(bf16).reshape(inner, slots, width)
        return lax.all_to_all(array, "inner", 0, 0, tiled=True).reshape(inner * slots, width)

    w_gate_up = jnp.concatenate([w_gate[0], w_up[0]], axis=1)
    inputs = to_experts(dot_nn(picks, normed_all))
    upstream_rows = to_experts(dot_nn(picks, upstream_all) * slot_gate)
    upstream_rows, w_whole, packed = lax.optimization_barrier((upstream_rows, w_whole, packed))
    pre = dot_nn(inputs, w_gate_up)
    gate_pre = pre[:, :ff]
    up_pre = pre[:, ff:]
    back_hidden = contract_last(upstream_rows, w_down[0])
    sigmoid = jax.nn.sigmoid(gate_pre)
    grad_gate = (back_hidden * up_pre * sigmoid * (1.0 + gate_pre * (1.0 - sigmoid))).astype(bf16)
    grad_up = (back_hidden * gate_pre * sigmoid).astype(bf16)
    grad_both = jnp.concatenate([grad_gate, grad_up], axis=1)

    half = width // HALVES
    sums = []
    for part in range(HALVES):
        grads = contract_last(grad_both, w_gate_up[part * half : (part + 1) * half])
        grads = grads.astype(bf16).reshape(inner, slots, half)
        grads = lax.all_to_all(grads, "inner", 0, 0, tiled=True).reshape(inner * slots, half)
        partial = contract_first(picks, grads).astype(bf16)
        sums.append(lax.psum_scatter(partial, "grp", scatter_dimension=0, tiled=True))

    packed, _ = lax.optimization_barrier((packed, partial))
    packed = lax.all_to_all(packed, "inner", 0, 0, tiled=True)
    packed = packed.reshape(inner * rows, head_width + 2 * HEAD_SIZE)
    packed, sums = lax.optimization_barrier((packed, sums))

    grad_normed = jnp.concatenate(sums, axis=1).astype(f32)

    gained = grad_normed * norm_gain
    statistic = jnp.mean(gained * hidden_f, axis=1, keepdims=True)
    grad_resid = (
        grad_out.astype(f32)
        + inverse * gained
        - hidden_f * inverse * inverse * inverse * statistic
    ).astype(bf16)

    heads = lse.shape[0]
    grads = []
    for head in range(heads):
        grad = project(grad_resid, w_whole, attn_out, head)
        grads.append(lax.all_to_all(grad, "inner", 0, 0, tiled=True))
    dkv = None
    token_query = []
    for head in range(heads - 1):
        dquery, dkv = attention(packed, grads[head], lse, head, dkv)
        dquery, grads[head + 1] = lax.optimization_barrier((dquery, grads[head + 1]))
        dquery = dquery.reshape(inner, rows, HEAD_SIZE)
        token_query.append(lax.all_to_all(dquery, "inner", 0, 0, tiled=True))
    (packed_grads,) = attention(packed, grads[-1], lse, heads - 1, dkv)
    packed_grads, token_query = lax.optimization_barrier((packed_grads, token_query))
    packed_grads = packed_grads.reshape(inner, rows, 3 * HEAD_SIZE)
    packed_grads = lax.all_to_all(packed_grads, "inner", 0, 0, tiled=True)
    token_query.append(packed_grads[:, :, :HEAD_SIZE])
    token_kv = packed_grads[:, :, HEAD_SIZE:]
    queries_gradient = jnp.concatenate(token_query, axis=2).transpose(1, 0, 2)
    queries_gradient = queries_gradient.reshape(rows, inner * head_width)
    totals = jnp.sum(
        token_kv.reshape(KEY_VALUE_HEADS, shared, rows, 2 * HEAD_SIZE).astype(f32), axis=1
    ).astype(bf16)
    kv_width = KEY_VALUE_HEADS * HEAD_SIZE
    keys_gradient = totals[:, :, :HEAD_SIZE].transpose(1, 0, 2).reshape(rows, kv_width)
    values_gradient = totals[:, :, HEAD_SIZE:].transpose(1, 0, 2).reshape(rows, kv_width)
    return (grad_resid, queries_gradient, keys_gradient, values_gradient)


def solution(mesh):
    token = P(("grp", "inner"), None)
    expert = P(("grp", "inner"), None, None)
    placed = (
        token,
        token,
        P(),
        token,
        token,
        expert,
        expert,
        expert,
        P("inner", None),
        token,
        token,
        token,
        token,
        P("inner", "grp"),
    )

    return jax.shard_map(
        per_device,
        mesh=mesh,
        in_specs=placed,
        out_specs=(token, token, token, token),
        check_vma=False,
    )
```

```python
import functools
import math

import jax
import jax.numpy as jnp
from jax import lax
from jax.experimental import pallas as pl
from jax.experimental.pallas import tpu as pltpu
from jax.sharding import PartitionSpec as P

KEY_VALUE_HEADS = 4
HEAD_SIZE = 128
EPSILON = 1e-06
BLOCK = 512
HALVES = 2
DELTA_ROWS = 16


def dot_nn(left, right):
    return lax.dot_general(
        left, right, (((1,), (0,)), ((), ())), preferred_element_type=jnp.float32
    )


def contract_last(left, right):
    return lax.dot_general(
        left, right, (((1,), (1,)), ((), ())), preferred_element_type=jnp.float32
    )


def contract_first(left, right):
    return lax.dot_general(
        left, right, (((0,), (0,)), ((), ())), preferred_element_type=jnp.float32
    )


def project_kernel(resid_ref, weight_ref, output_ref, out_ref, *, head):
    parts, devices = weight_ref.shape[:2]
    piece = weight_ref.shape[3]
    total = None
    for part in range(parts):
        weight = weight_ref[part].reshape(devices * HEAD_SIZE, piece)
        term = contract_last(weight, resid_ref[:, part * piece : (part + 1) * piece])
        total = term if total is None else total + term
    head_width = output_ref.shape[1] // devices
    row_at = lax.broadcasted_iota(jnp.int32, (DELTA_ROWS, resid_ref.shape[0]), 0)
    for device in range(devices):
        grad = total[device * HEAD_SIZE : (device + 1) * HEAD_SIZE].astype(jnp.bfloat16)
        start = device * head_width + head * HEAD_SIZE
        output = output_ref[:, start : start + HEAD_SIZE].astype(jnp.float32).T
        rest = jnp.sum(grad.astype(jnp.float32) * output, axis=0, keepdims=True)
        held = jnp.zeros(row_at.shape, jnp.float32)
        for row in range(3):
            digit = rest.astype(jnp.bfloat16).astype(jnp.float32)
            held = jnp.where(row_at == row, digit, held)
            rest = rest - digit
        out_ref[device, :HEAD_SIZE] = grad
        out_ref[device, HEAD_SIZE:] = held.astype(jnp.bfloat16)


def project(resid, weights, attn_out, head):
    tokens, width = resid.shape
    parts, devices, heads, _, piece = weights.shape
    step = min(4, devices)
    head_rows = HEAD_SIZE + DELTA_ROWS
    return pl.pallas_call(
        functools.partial(project_kernel, head=head),
        grid=(devices // step,),
        in_specs=[
            pl.BlockSpec((tokens, width), lambda n: (0, 0)),
            pl.BlockSpec(
                (parts, step, None, HEAD_SIZE, piece), lambda n: (0, n, head, 0, 0)
            ),
            pl.BlockSpec((tokens, step * heads * HEAD_SIZE), lambda n: (0, n)),
        ],
        out_specs=pl.BlockSpec((step, head_rows, tokens), lambda n: (n, 0, 0)),
        out_shape=jax.ShapeDtypeStruct((devices, head_rows, tokens), jnp.bfloat16),
        cost_estimate=pl.CostEstimate(
            flops=2 * tokens * width * devices * HEAD_SIZE,
            bytes_accessed=2 * devices * HEAD_SIZE * (width + 3 * tokens),
            transcendentals=0,
        ),
    )(resid, weights, attn_out)


def attention_kernel(packed_ref, grad_ref, lse_ref, *refs, head, heads):
    last = head == heads - 1
    before_ref = refs[0] if head > 0 else None
    if last:
        out_ref, delta_ref, grad_t_ref, dqt_ref = refs[-4:]
    else:
        dquery_ref, dkv_ref, delta_ref, grad_t_ref, dqt_ref = refs[-5:]
    j = pl.program_id(0)
    steps = pl.num_programs(0)
    length = packed_ref.shape[0]
    devices, _, tokens = grad_ref.shape
    block = min(BLOCK, length)
    scale = float(HEAD_SIZE) ** (-0.5)
    log2e = math.log2(math.e)
    key_from = heads * HEAD_SIZE
    value_from = key_from + HEAD_SIZE
    query_cols = slice(head * HEAD_SIZE, (head + 1) * HEAD_SIZE)

    @pl.when(j == 0)
    def _():
        dqt_ref[...] = jnp.zeros_like(dqt_ref)
        for device in range(devices):
            cols = slice(device * tokens, (device + 1) * tokens)
            grad_t_ref[:, cols] = grad_ref[device, :HEAD_SIZE]
            digits = grad_ref[device, HEAD_SIZE:].astype(jnp.float32)
            delta_ref[:, cols] = jnp.broadcast_to(
                jnp.sum(digits, axis=0, keepdims=True), (8, tokens)
            )

    key_rows = pl.ds(pl.multiple_of(j * block, block), block)
    key = packed_ref[key_rows, key_from:value_from]
    value = packed_ref[key_rows, value_from : value_from + HEAD_SIZE]
    key_t = key.astype(jnp.float32).T.astype(jnp.bfloat16)

    def one(i):
        rows = pl.ds(pl.multiple_of(i * block, block), block)
        query = packed_ref[rows, query_cols]
        grad_t = grad_t_ref[:, rows]
        lse = lse_ref[head : head + 1, rows] * log2e
        delta = delta_ref[0:1, rows]
        scores = contract_last(key, query)
        probs = jnp.exp2(scores * (scale * log2e) - lse)
        key_at = j * block + lax.broadcasted_iota(jnp.int32, scores.shape, 0)
        query_at = i * block + lax.broadcasted_iota(jnp.int32, scores.shape, 1)
        probs = jnp.where(key_at <= query_at, probs, 0.0)
        grad_probs = dot_nn(value, grad_t)
        grad_scores = (probs * (grad_probs - delta)).astype(jnp.bfloat16)
        dkey = dot_nn(grad_scores, query)
        dvalue = contract_last(probs.astype(jnp.bfloat16), grad_t)
        dqt_ref[:, rows] += dot_nn(key_t, grad_scores)
        return dkey, dvalue

    def body(i, carry):
        dkey, dvalue = one(i)
        return carry[0] + dkey, carry[1] + dvalue

    zero = jnp.zeros((block, HEAD_SIZE), jnp.float32)
    dkey, dvalue = lax.fori_loop(j, steps, body, (zero, zero))
    dkey = dkey * scale
    if before_ref is not None:
        dkey = dkey + before_ref[key_rows, :HEAD_SIZE]
        dvalue = dvalue + before_ref[key_rows, HEAD_SIZE:]
    if last:
        out_ref[key_rows, HEAD_SIZE : 2 * HEAD_SIZE] = dkey.astype(jnp.bfloat16)
        out_ref[key_rows, 2 * HEAD_SIZE :] = dvalue.astype(jnp.bfloat16)
    else:
        dkv_ref[key_rows, :HEAD_SIZE] = dkey
        dkv_ref[key_rows, HEAD_SIZE:] = dvalue

    @pl.when(j == steps - 1)
    def _():
        dquery = (dqt_ref[...].T * scale).astype(jnp.bfloat16)
        if last:
            out_ref[:, :HEAD_SIZE] = dquery
        else:
            dquery_ref[...] = dquery


def attention(packed, grad, lse, head, before):
    length, packed_width = packed.shape
    heads = lse.shape[0]
    last = head == heads - 1
    block = min(BLOCK, length)
    operands = [packed, grad, lse] + ([before] if head > 0 else [])

    def whole(shape):
        return pl.BlockSpec(shape, lambda j: (0,) * len(shape))

    if last:
        shapes = [jax.ShapeDtypeStruct((length, 3 * HEAD_SIZE), jnp.bfloat16)]
    else:
        shapes = [
            jax.ShapeDtypeStruct((length, HEAD_SIZE), jnp.bfloat16),
            jax.ShapeDtypeStruct((length, 2 * HEAD_SIZE), jnp.float32),
        ]
    return pl.pallas_call(
        functools.partial(attention_kernel, head=head, heads=heads),
        grid=(length // block,),
        in_specs=[whole(operand.shape) for operand in operands],
        out_specs=[whole(shape.shape) for shape in shapes],
        out_shape=shapes,
        scratch_shapes=[
            pltpu.VMEM((8, length), jnp.float32),
            pltpu.VMEM((HEAD_SIZE, length), jnp.bfloat16),
            pltpu.VMEM((HEAD_SIZE, length), jnp.float32),
        ],
        compiler_params=pltpu.CompilerParams(
            dimension_semantics=("arbitrary",), vmem_limit_bytes=48 * 1024 * 1024
        ),
        cost_estimate=pl.CostEstimate(
            flops=10 * length * length * HEAD_SIZE // 2,
            bytes_accessed=2 * length * (packed_width + 6 * HEAD_SIZE),
            transcendentals=length * length // 2,
        ),
    )(*operands)


def per_device(
    grad_out,
    hidden,
    norm_gain,
    expert_ids,
    gate_weights,
    w_gate,
    w_up,
    w_down,
    w_out,
    queries,
    keys,
    values,
    attn_out,
    lse,
):
    bf16, f32 = jnp.bfloat16, jnp.float32
    rows, width = hidden.shape
    topk = expert_ids.shape[1]
    groups = lax.axis_size("grp")
    inner = lax.axis_size("inner")
    grp_at = lax.axis_index("grp")
    experts = groups * inner
    capacity = max(2, 5 * rows * topk // (4 * experts))
    slots = groups * capacity
    column = groups * rows
    ff = w_gate.shape[2]
    head_width = queries.shape[1] // inner
    shared = inner // KEY_VALUE_HEADS

    hidden_f = hidden.astype(f32)
    inverse = lax.rsqrt(jnp.mean(hidden_f * hidden_f, axis=1, keepdims=True) + EPSILON)
    normed = (hidden_f * inverse * norm_gain).astype(bf16)

    normed_all = lax.all_gather(normed, "grp", axis=0, tiled=True)
    upstream_all = lax.all_gather(grad_out, "grp", axis=0, tiled=True)
    routing = jnp.concatenate([expert_ids.astype(f32).T, gate_weights.T], axis=0)
    routing = lax.all_gather(routing, "grp", axis=0, tiled=False)

    piece = width // groups
    w_piece = lax.dynamic_slice_in_dim(w_out, grp_at * piece, piece, axis=1)
    w_piece = jnp.broadcast_to(w_piece[None], (inner,) + w_piece.shape)
    w_piece = lax.all_to_all(w_piece, "inner", 0, 0, tiled=True)
    normed_all, w_piece = lax.optimization_barrier((normed_all, w_piece))
    w_whole = lax.all_gather(w_piece, "grp", axis=0, tiled=False)
    w_whole = w_whole.reshape(groups, inner, head_width // HEAD_SIZE, HEAD_SIZE, piece)

    kv = jnp.stack(
        [
            keys.reshape(rows, KEY_VALUE_HEADS, HEAD_SIZE),
            values.reshape(rows, KEY_VALUE_HEADS, HEAD_SIZE),
        ],
        axis=2,
    ).reshape(rows, KEY_VALUE_HEADS, 2 * HEAD_SIZE)
    kv = jnp.repeat(kv.transpose(1, 0, 2), shared, axis=0)
    packed = jnp.concatenate(
        [queries.reshape(rows, inner, head_width).transpose(1, 0, 2), kv], axis=2
    )

    ids_all = routing[:, :topk]
    gates_all = routing[:, topk:]
    mine = (grp_at * inner + lax.broadcasted_iota(jnp.int32, (1, inner, 1, 1), 1)).astype(f32)
    match = ids_all[:, None] == mine
    named = jnp.any(match, axis=2)
    gate = jnp.sum(jnp.where(match, gates_all[:, None], 0.0), axis=2)
    before = (
        lax.broadcasted_iota(jnp.int32, (rows, rows), 0)
        < lax.broadcasted_iota(jnp.int32, (rows, rows), 1)
    ).astype(bf16)
    rank = dot_nn(named.astype(bf16).reshape(groups * inner, rows), before)
    rank = rank.reshape(groups, inner, rows)
    block_at = lax.broadcasted_iota(jnp.int32, (groups, 1, 1), 0).astype(f32)
    slot = jnp.where(named, block_at * capacity + rank, -1.0)
    slot = slot.transpose(1, 0, 2).reshape(inner, 1, column)
    gate = gate.transpose(1, 0, 2).reshape(inner, 1, column)
    slot_at = lax.broadcasted_iota(jnp.int32, (1, slots, 1), 1).astype(f32)
    chosen = slot == slot_at
    picks = jnp.where(slot == slot_at, 1.0, 0.0).astype(bf16).reshape(inner * slots, column)
    picks = lax.optimization_barrier(picks)
    slot_gate = jnp.sum(jnp.where(chosen, gate, 0.0), axis=2).reshape(inner * slots, 1)

    def to_experts(array):
        array = array.astype(bf16).reshape(inner, slots, width)
        return lax.all_to_all(array, "inner", 0, 0, tiled=True).reshape(inner * slots, width)

    w_gate_up = jnp.concatenate([w_gate[0], w_up[0]], axis=1)
    inputs = to_experts(dot_nn(picks, normed_all))
    upstream_rows = to_experts(dot_nn(picks, upstream_all) * slot_gate)
    pre = dot_nn(inputs, w_gate_up)
    gate_pre = pre[:, :ff]
    up_pre = pre[:, ff:]
    sigmoid = jax.nn.sigmoid(gate_pre)
    gate_slope = up_pre * sigmoid * (1.0 + gate_pre * (1.0 - sigmoid))
    up_slope = gate_pre * sigmoid
    half = width // HALVES
    w_halves = [
        jnp.concatenate([w[0, part * half : (part + 1) * half] for w in (w_gate, w_up)], axis=1)
        for part in range(HALVES)
    ]
    upstream_rows, w_whole, packed, gate_slope, up_slope, w_halves = lax.optimization_barrier(
        (upstream_rows, w_whole, packed, gate_slope, up_slope, w_halves)
    )
    back_hidden = contract_last(upstream_rows, w_down[0])
    grad_gate = (back_hidden * gate_slope).astype(bf16)
    grad_up = (back_hidden * up_slope).astype(bf16)
    grad_both = jnp.concatenate([grad_gate, grad_up], axis=1)

    def add_up(rows_back):
        return contract_first(picks, rows_back.reshape(inner * slots, half)).astype(bf16)

    sums = []
    grads = []
    for part in range(HALVES):
        grads.append(contract_last(grad_both, w_halves[part]))
        grads[part] = grads[part].astype(bf16).reshape(inner, slots, half)
    for part in range(HALVES):
        if part > 0:
            returned, grads[part] = lax.optimization_barrier((returned, grads[part]))
        arrived = lax.all_to_all(grads[part], "inner", 0, 0, tiled=True)
        if part > 0:
            sums.append(lax.psum_scatter(add_up(returned), "grp", scatter_dimension=0, tiled=True))
        returned = arrived
    partial = add_up(returned)
    sums.append(lax.psum_scatter(partial, "grp", scatter_dimension=0, tiled=True))

    packed, _ = lax.optimization_barrier((packed, partial))
    packed = lax.all_to_all(packed, "inner", 0, 0, tiled=True)
    packed = packed.reshape(inner * rows, head_width + 2 * HEAD_SIZE)
    packed, sums = lax.optimization_barrier((packed, sums))

    grad_normed = jnp.concatenate(sums, axis=1).astype(f32)

    gained = grad_normed * norm_gain
    statistic = jnp.mean(gained * hidden_f, axis=1, keepdims=True)
    grad_resid = (
        grad_out.astype(f32)
        + inverse * gained
        - hidden_f * inverse * inverse * inverse * statistic
    ).astype(bf16)

    heads = lse.shape[0]
    grads = []
    for head in range(heads):
        grad = project(grad_resid, w_whole, attn_out, head)
        grads.append(lax.all_to_all(grad, "inner", 0, 0, tiled=True))
    dkv = None
    token_query = []
    for head in range(heads - 1):
        dquery, dkv = attention(packed, grads[head], lse, head, dkv)
        dquery, grads[head + 1] = lax.optimization_barrier((dquery, grads[head + 1]))
        dquery = dquery.reshape(inner, rows, HEAD_SIZE)
        token_query.append(lax.all_to_all(dquery, "inner", 0, 0, tiled=True))
    (packed_grads,) = attention(packed, grads[-1], lse, heads - 1, dkv)
    packed_grads, token_query = lax.optimization_barrier((packed_grads, token_query))
    packed_grads = packed_grads.reshape(inner, rows, 3 * HEAD_SIZE)
    packed_grads = lax.all_to_all(packed_grads, "inner", 0, 0, tiled=True)
    token_query.append(packed_grads[:, :, :HEAD_SIZE])
    token_kv = packed_grads[:, :, HEAD_SIZE:]
    queries_gradient = jnp.concatenate(token_query, axis=2).transpose(1, 0, 2)
    queries_gradient = queries_gradient.reshape(rows, inner * head_width)
    totals = jnp.sum(
        token_kv.reshape(KEY_VALUE_HEADS, shared, rows, 2 * HEAD_SIZE).astype(f32), axis=1
    ).astype(bf16)
    kv_width = KEY_VALUE_HEADS * HEAD_SIZE
    keys_gradient = totals[:, :, :HEAD_SIZE].transpose(1, 0, 2).reshape(rows, kv_width)
    values_gradient = totals[:, :, HEAD_SIZE:].transpose(1, 0, 2).reshape(rows, kv_width)
    return (grad_resid, queries_gradient, keys_gradient, values_gradient)


def solution(mesh):
    token = P(("grp", "inner"), None)
    expert = P(("grp", "inner"), None, None)
    placed = (
        token,
        token,
        P(),
        token,
        token,
        expert,
        expert,
        expert,
        P("inner", None),
        token,
        token,
        token,
        token,
        P("inner", "grp"),
    )

    return jax.shard_map(
        per_device,
        mesh=mesh,
        in_specs=placed,
        out_specs=(token, token, token, token),
        check_vma=False,
    )
```

```python
import functools
import math

import jax
import jax.numpy as jnp
from jax import lax
from jax.experimental import pallas as pl
from jax.experimental.pallas import tpu as pltpu
from jax.sharding import PartitionSpec as P

KEY_VALUE_HEADS = 4
HEAD_SIZE = 128
EPSILON = 1e-06
BLOCK = 512
HALVES = 2
DELTA_ROWS = 16


def dot_nn(left, right):
    return lax.dot_general(
        left, right, (((1,), (0,)), ((), ())), preferred_element_type=jnp.float32
    )


def contract_last(left, right):
    return lax.dot_general(
        left, right, (((1,), (1,)), ((), ())), preferred_element_type=jnp.float32
    )


def contract_first(left, right):
    return lax.dot_general(
        left, right, (((0,), (0,)), ((), ())), preferred_element_type=jnp.float32
    )


def project_kernel(resid_ref, weight_ref, output_ref, out_ref, *, head):
    parts, devices = weight_ref.shape[:2]
    piece = weight_ref.shape[3]
    total = None
    for part in range(parts):
        weight = weight_ref[part].reshape(devices * HEAD_SIZE, piece)
        term = contract_last(weight, resid_ref[:, part * piece : (part + 1) * piece])
        total = term if total is None else total + term
    head_width = output_ref.shape[1] // devices
    row_at = lax.broadcasted_iota(jnp.int32, (DELTA_ROWS, resid_ref.shape[0]), 0)
    for device in range(devices):
        grad = total[device * HEAD_SIZE : (device + 1) * HEAD_SIZE].astype(jnp.bfloat16)
        start = device * head_width + head * HEAD_SIZE
        output = output_ref[:, start : start + HEAD_SIZE].astype(jnp.float32).T
        rest = jnp.sum(grad.astype(jnp.float32) * output, axis=0, keepdims=True)
        held = jnp.zeros(row_at.shape, jnp.float32)
        for row in range(3):
            digit = rest.astype(jnp.bfloat16).astype(jnp.float32)
            held = jnp.where(row_at == row, digit, held)
            rest = rest - digit
        out_ref[device, :HEAD_SIZE] = grad
        out_ref[device, HEAD_SIZE:] = held.astype(jnp.bfloat16)


def project(resid, weights, attn_out, head):
    tokens, width = resid.shape
    parts, devices, heads, _, piece = weights.shape
    step = min(4, devices)
    head_rows = HEAD_SIZE + DELTA_ROWS
    return pl.pallas_call(
        functools.partial(project_kernel, head=head),
        grid=(devices // step,),
        in_specs=[
            pl.BlockSpec((tokens, width), lambda n: (0, 0)),
            pl.BlockSpec(
                (parts, step, None, HEAD_SIZE, piece), lambda n: (0, n, head, 0, 0)
            ),
            pl.BlockSpec((tokens, step * heads * HEAD_SIZE), lambda n: (0, n)),
        ],
        out_specs=pl.BlockSpec((step, head_rows, tokens), lambda n: (n, 0, 0)),
        out_shape=jax.ShapeDtypeStruct((devices, head_rows, tokens), jnp.bfloat16),
        cost_estimate=pl.CostEstimate(
            flops=2 * tokens * width * devices * HEAD_SIZE,
            bytes_accessed=2 * devices * HEAD_SIZE * (width + 3 * tokens),
            transcendentals=0,
        ),
    )(resid, weights, attn_out)


def attention_kernel(packed_ref, grad_ref, lse_ref, *refs, head, heads):
    last = head == heads - 1
    before_ref = refs[0] if head > 0 else None
    if last:
        out_ref, delta_ref, grad_t_ref, dqt_ref = refs[-4:]
    else:
        dquery_ref, dkv_ref, delta_ref, grad_t_ref, dqt_ref = refs[-5:]
    j = pl.program_id(0)
    steps = pl.num_programs(0)
    length = packed_ref.shape[0]
    devices, _, tokens = grad_ref.shape
    block = min(BLOCK, length)
    scale = float(HEAD_SIZE) ** (-0.5)
    log2e = math.log2(math.e)
    key_from = heads * HEAD_SIZE
    value_from = key_from + HEAD_SIZE
    query_cols = slice(head * HEAD_SIZE, (head + 1) * HEAD_SIZE)

    @pl.when(j == 0)
    def _():
        dqt_ref[...] = jnp.zeros_like(dqt_ref)
        for device in range(devices):
            cols = slice(device * tokens, (device + 1) * tokens)
            grad_t_ref[:, cols] = grad_ref[device, :HEAD_SIZE]
            digits = grad_ref[device, HEAD_SIZE:].astype(jnp.float32)
            delta_ref[:, cols] = jnp.broadcast_to(
                jnp.sum(digits, axis=0, keepdims=True), (8, tokens)
            )

    key_rows = pl.ds(pl.multiple_of(j * block, block), block)
    key = packed_ref[key_rows, key_from:value_from]
    value = packed_ref[key_rows, value_from : value_from + HEAD_SIZE]
    key_t = key.astype(jnp.float32).T.astype(jnp.bfloat16)

    def one(i):
        rows = pl.ds(pl.multiple_of(i * block, block), block)
        query = packed_ref[rows, query_cols]
        grad_t = grad_t_ref[:, rows]
        lse = lse_ref[head : head + 1, rows] * log2e
        delta = delta_ref[0:1, rows]
        scores = contract_last(key, query)
        probs = jnp.exp2(scores * (scale * log2e) - lse)
        key_at = j * block + lax.broadcasted_iota(jnp.int32, scores.shape, 0)
        query_at = i * block + lax.broadcasted_iota(jnp.int32, scores.shape, 1)
        probs = jnp.where(key_at <= query_at, probs, 0.0)
        grad_probs = dot_nn(value, grad_t)
        grad_scores = (probs * (grad_probs - delta)).astype(jnp.bfloat16)
        dkey = dot_nn(grad_scores, query)
        dvalue = contract_last(probs.astype(jnp.bfloat16), grad_t)
        dqt_ref[:, rows] += dot_nn(key_t, grad_scores)
        return dkey, dvalue

    def body(i, carry):
        dkey, dvalue = one(i)
        return carry[0] + dkey, carry[1] + dvalue

    zero = jnp.zeros((block, HEAD_SIZE), jnp.float32)
    dkey, dvalue = lax.fori_loop(j, steps, body, (zero, zero))
    dkey = dkey * scale
    if before_ref is not None:
        dkey = dkey + before_ref[key_rows, :HEAD_SIZE]
        dvalue = dvalue + before_ref[key_rows, HEAD_SIZE:]
    if last:
        out_ref[key_rows, HEAD_SIZE : 2 * HEAD_SIZE] = dkey.astype(jnp.bfloat16)
        out_ref[key_rows, 2 * HEAD_SIZE :] = dvalue.astype(jnp.bfloat16)
    else:
        dkv_ref[key_rows, :HEAD_SIZE] = dkey
        dkv_ref[key_rows, HEAD_SIZE:] = dvalue

    @pl.when(j == steps - 1)
    def _():
        dquery = (dqt_ref[...].T * scale).astype(jnp.bfloat16)
        if last:
            out_ref[:, :HEAD_SIZE] = dquery
        else:
            dquery_ref[...] = dquery


def attention(packed, grad, lse, head, before):
    length, packed_width = packed.shape
    heads = lse.shape[0]
    last = head == heads - 1
    block = min(BLOCK, length)
    operands = [packed, grad, lse] + ([before] if head > 0 else [])

    def whole(shape):
        return pl.BlockSpec(shape, lambda j: (0,) * len(shape))

    if last:
        shapes = [jax.ShapeDtypeStruct((length, 3 * HEAD_SIZE), jnp.bfloat16)]
    else:
        shapes = [
            jax.ShapeDtypeStruct((length, HEAD_SIZE), jnp.bfloat16),
            jax.ShapeDtypeStruct((length, 2 * HEAD_SIZE), jnp.float32),
        ]
    return pl.pallas_call(
        functools.partial(attention_kernel, head=head, heads=heads),
        grid=(length // block,),
        in_specs=[whole(operand.shape) for operand in operands],
        out_specs=[whole(shape.shape) for shape in shapes],
        out_shape=shapes,
        scratch_shapes=[
            pltpu.VMEM((8, length), jnp.float32),
            pltpu.VMEM((HEAD_SIZE, length), jnp.bfloat16),
            pltpu.VMEM((HEAD_SIZE, length), jnp.float32),
        ],
        compiler_params=pltpu.CompilerParams(
            dimension_semantics=("arbitrary",), vmem_limit_bytes=48 * 1024 * 1024
        ),
        cost_estimate=pl.CostEstimate(
            flops=10 * length * length * HEAD_SIZE // 2,
            bytes_accessed=2 * length * (packed_width + 6 * HEAD_SIZE),
            transcendentals=length * length // 2,
        ),
    )(*operands)


def gather_kernel(picks_ref, table_ref, out_ref):
    rows = dot_nn(picks_ref[...], table_ref[...]).astype(jnp.bfloat16)
    out_ref[...] = rows.reshape(out_ref.shape)


def gather(picks, table, devices):
    slots, tokens = picks.shape
    width = table.shape[1]
    piece = min(256, width)
    out = (devices, slots // devices, width)
    return pl.pallas_call(
        gather_kernel,
        grid=(width // piece,),
        in_specs=[
            pl.BlockSpec((slots, tokens), lambda n: (0, 0)),
            pl.BlockSpec((tokens, piece), lambda n: (0, n)),
        ],
        out_specs=pl.BlockSpec(out[:2] + (piece,), lambda n: (0, 0, n)),
        out_shape=jax.ShapeDtypeStruct(out, jnp.bfloat16),
        cost_estimate=pl.CostEstimate(
            flops=2 * slots * tokens * width,
            bytes_accessed=2 * (slots * tokens + (tokens + slots) * width),
            transcendentals=0,
        ),
        name="gather",
    )(picks, table)


def assemble_kernel(*refs):
    earlier, packed_ref = refs[:-4], refs[-4]
    query_ref, key_ref, value_ref = refs[-3:]
    devices = packed_ref.shape[0]
    heads = len(earlier) + 1
    total = packed_ref[0, :, HEAD_SIZE:].astype(jnp.float32)
    for device in range(1, devices):
        total = total + packed_ref[device, :, HEAD_SIZE:].astype(jnp.float32)
    key_ref[...] = total[:, :HEAD_SIZE].astype(jnp.bfloat16)
    value_ref[...] = total[:, HEAD_SIZE:].astype(jnp.bfloat16)
    for device in range(devices):
        for head in range(heads):
            start = (device * heads + head) * HEAD_SIZE
            part = packed_ref[device, :, :HEAD_SIZE]
            if head < heads - 1:
                part = earlier[head][device]
            query_ref[:, start : start + HEAD_SIZE] = part


def assemble(earlier, packed):
    devices, rows, packed_width = packed.shape
    shared = devices // KEY_VALUE_HEADS
    heads = len(earlier) + 1
    query_width = shared * heads * HEAD_SIZE
    bf16 = jnp.bfloat16
    return pl.pallas_call(
        assemble_kernel,
        grid=(KEY_VALUE_HEADS,),
        in_specs=[pl.BlockSpec((shared, rows, HEAD_SIZE), lambda n: (n, 0, 0))] * (heads - 1)
        + [pl.BlockSpec((shared, rows, packed_width), lambda n: (n, 0, 0))],
        out_specs=[
            pl.BlockSpec((rows, query_width), lambda n: (0, n)),
            pl.BlockSpec((rows, HEAD_SIZE), lambda n: (0, n)),
            pl.BlockSpec((rows, HEAD_SIZE), lambda n: (0, n)),
        ],
        out_shape=[
            jax.ShapeDtypeStruct((rows, KEY_VALUE_HEADS * query_width), bf16),
            jax.ShapeDtypeStruct((rows, KEY_VALUE_HEADS * HEAD_SIZE), bf16),
            jax.ShapeDtypeStruct((rows, KEY_VALUE_HEADS * HEAD_SIZE), bf16),
        ],
        name="assemble",
    )(*earlier, packed)


def pick(array, index, axis):
    starts = [jnp.int32(0)] * array.ndim
    starts[axis] = index.astype(jnp.int32)
    sizes = list(array.shape)
    sizes[axis] = 1
    piece = lax.dynamic_slice(array, starts, sizes, allow_negative_indices=False)
    return lax.squeeze(piece, (axis,))


def scatter_sum(partial, groups, rows):
    grp_at = lax.axis_index("grp")
    core = lax.rem(grp_at, 2)
    place = lax.div(grp_at, 2)
    chips = groups // 2
    f32 = jnp.float32
    parts = partial.reshape(chips, 2, rows, partial.shape[1])
    keep = pick(parts, core, 1)
    send = pick(parts, 1 - core, 1)
    other = lax.ppermute(send, "grp", [(g, g ^ 1) for g in range(groups)])
    pair = (keep.astype(f32) + other.astype(f32)).astype(jnp.bfloat16)
    total = pick(pair, place, 0).astype(f32)
    for step in range(1, chips):
        block = pick(pair, lax.rem(place + step, chips), 0)
        moves = [(g, (g // 2 + step) % chips * 2 + g % 2) for g in range(groups)]
        block = lax.ppermute(block, "grp", moves)
        total = total + block.astype(f32)
    return total


def per_device(
    grad_out,
    hidden,
    norm_gain,
    expert_ids,
    gate_weights,
    w_gate,
    w_up,
    w_down,
    w_out,
    queries,
    keys,
    values,
    attn_out,
    lse,
):
    bf16, f32 = jnp.bfloat16, jnp.float32
    rows, width = hidden.shape
    topk = expert_ids.shape[1]
    groups = lax.axis_size("grp")
    inner = lax.axis_size("inner")
    grp_at = lax.axis_index("grp")
    experts = groups * inner
    capacity = max(2, 5 * rows * topk // (4 * experts))
    slots = groups * capacity
    column = groups * rows
    ff = w_gate.shape[2]
    head_width = queries.shape[1] // inner
    shared = inner // KEY_VALUE_HEADS

    hidden_f = hidden.astype(f32)
    inverse = lax.rsqrt(jnp.mean(hidden_f * hidden_f, axis=1, keepdims=True) + EPSILON)
    normed = (hidden_f * inverse * norm_gain).astype(bf16)

    normed_all = lax.all_gather(normed, "grp", axis=0, tiled=True)
    upstream_all = lax.all_gather(grad_out, "grp", axis=0, tiled=True)
    routing = jnp.concatenate([expert_ids.astype(f32).T, gate_weights.T], axis=0)
    routing = lax.all_gather(routing, "grp", axis=0, tiled=False)

    piece = width // groups
    w_piece = lax.dynamic_slice_in_dim(w_out, grp_at * piece, piece, axis=1)
    w_piece = jnp.broadcast_to(w_piece[None], (inner,) + w_piece.shape)
    w_piece = lax.all_to_all(w_piece, "inner", 0, 0, tiled=True)
    normed_all, w_piece = lax.optimization_barrier((normed_all, w_piece))
    w_whole = lax.all_gather(w_piece, "grp", axis=0, tiled=False)
    w_whole = w_whole.reshape(groups, inner, head_width // HEAD_SIZE, HEAD_SIZE, piece)

    ids_all = routing[:, :topk]
    gates_all = routing[:, topk:]
    mine = (grp_at * inner + lax.broadcasted_iota(jnp.int32, (1, inner, 1, 1), 1)).astype(f32)
    match = ids_all[:, None] == mine
    named = jnp.any(match, axis=2)
    gate = jnp.sum(jnp.where(match, gates_all[:, None], 0.0), axis=2)
    before = (
        lax.broadcasted_iota(jnp.int32, (rows, rows), 0)
        < lax.broadcasted_iota(jnp.int32, (rows, rows), 1)
    ).astype(bf16)
    rank = dot_nn(named.astype(bf16).reshape(groups * inner, rows), before)
    rank = rank.reshape(groups, inner, rows)
    block_at = lax.broadcasted_iota(jnp.int32, (groups, 1, 1), 0).astype(f32)
    slot = jnp.where(named, block_at * capacity + rank, -1.0)
    slot = slot.transpose(1, 0, 2).reshape(inner, 1, column)
    gate = gate.transpose(1, 0, 2).reshape(inner, 1, column)
    slot_at = lax.broadcasted_iota(jnp.int32, (1, slots, 1), 1).astype(f32)
    chosen = slot == slot_at
    picks = jnp.where(slot == slot_at, 1.0, 0.0).astype(bf16).reshape(inner * slots, column)
    picks = lax.optimization_barrier(picks)

    def to_experts(array):
        return lax.all_to_all(array, "inner", 0, 0, tiled=True).reshape(inner * slots, width)

    slot_gate = jnp.sum(jnp.where(chosen, gate, 0.0), axis=2)
    inputs = to_experts(gather(picks, normed_all, inner))
    slot_gate = slot_gate.reshape(inner * slots, 1)
    upstream_rows = (dot_nn(picks, upstream_all) * slot_gate).astype(bf16)
    upstream_rows = to_experts(upstream_rows.reshape(inner, slots, width))

    kv = jnp.stack(
        [
            keys.reshape(rows, KEY_VALUE_HEADS, HEAD_SIZE),
            values.reshape(rows, KEY_VALUE_HEADS, HEAD_SIZE),
        ],
        axis=2,
    ).reshape(rows, KEY_VALUE_HEADS, 2 * HEAD_SIZE)
    kv = jnp.repeat(kv.transpose(1, 0, 2), shared, axis=0)
    packed = jnp.concatenate(
        [queries.reshape(rows, inner, head_width).transpose(1, 0, 2), kv], axis=2
    )

    w_gate_up = jnp.concatenate([w_gate[0], w_up[0]], axis=1)
    pre = dot_nn(inputs, w_gate_up)
    gate_pre = pre[:, :ff]
    up_pre = pre[:, ff:]
    sigmoid = jax.nn.sigmoid(gate_pre)
    gate_slope = up_pre * sigmoid * (1.0 + gate_pre * (1.0 - sigmoid))
    up_slope = gate_pre * sigmoid
    half = width // HALVES
    w_halves = [
        jnp.concatenate([w[0, part * half : (part + 1) * half] for w in (w_gate, w_up)], axis=1)
        for part in range(HALVES)
    ]
    upstream_rows, w_whole, packed, gate_slope, up_slope, w_halves = lax.optimization_barrier(
        (upstream_rows, w_whole, packed, gate_slope, up_slope, w_halves)
    )
    back_hidden = contract_last(upstream_rows, w_down[0])
    grad_gate = (back_hidden * gate_slope).astype(bf16)
    grad_up = (back_hidden * up_slope).astype(bf16)
    grad_both = jnp.concatenate([grad_gate, grad_up], axis=1)

    def add_up(rows_back):
        return contract_first(picks, rows_back.reshape(inner * slots, half)).astype(bf16)

    sums = []
    grads = []
    for part in range(HALVES):
        grads.append(contract_last(grad_both, w_halves[part]))
        grads[part] = grads[part].astype(bf16).reshape(inner, slots, half)
    for part in range(HALVES):
        if part > 0:
            returned, grads[part] = lax.optimization_barrier((returned, grads[part]))
        arrived = lax.all_to_all(grads[part], "inner", 0, 0, tiled=True)
        if part > 0:
            sums.append(scatter_sum(add_up(returned), groups, rows))
        returned = arrived
    packed, returned = lax.optimization_barrier((packed, returned))
    packed = lax.all_to_all(packed, "inner", 0, 0, tiled=True)
    packed = packed.reshape(inner * rows, head_width + 2 * HEAD_SIZE)
    sums.append(scatter_sum(add_up(returned), groups, rows))
    grad_normed = jnp.concatenate(sums, axis=1)

    gained = grad_normed * norm_gain
    statistic = jnp.mean(gained * hidden_f, axis=1, keepdims=True)
    grad_resid = (
        grad_out.astype(f32)
        + inverse * gained
        - hidden_f * inverse * inverse * inverse * statistic
    ).astype(bf16)

    heads = lse.shape[0]
    grads = []
    for head in range(heads):
        grad = project(grad_resid, w_whole, attn_out, head)
        if head == 0:
            grad, packed = lax.optimization_barrier((grad, packed))
        grads.append(lax.all_to_all(grad, "inner", 0, 0, tiled=True))
    dkv = None
    token_query = []
    for head in range(heads - 1):
        dquery, dkv = attention(packed, grads[head], lse, head, dkv)
        dquery, grads[head + 1] = lax.optimization_barrier((dquery, grads[head + 1]))
        dquery = dquery.reshape(inner, rows, HEAD_SIZE)
        token_query.append(lax.all_to_all(dquery, "inner", 0, 0, tiled=True))
    (packed_grads,) = attention(packed, grads[-1], lse, heads - 1, dkv)
    packed_grads, token_query = lax.optimization_barrier((packed_grads, token_query))
    packed_grads = packed_grads.reshape(inner, rows, 3 * HEAD_SIZE)
    packed_grads = lax.all_to_all(packed_grads, "inner", 0, 0, tiled=True)
    queries_gradient, keys_gradient, values_gradient = assemble(token_query, packed_grads)
    return (grad_resid, queries_gradient, keys_gradient, values_gradient)


def solution(mesh):
    token = P(("grp", "inner"), None)
    expert = P(("grp", "inner"), None, None)
    placed = (
        token,
        token,
        P(),
        token,
        token,
        expert,
        expert,
        expert,
        P("inner", None),
        token,
        token,
        token,
        token,
        P("inner", "grp"),
    )

    return jax.shard_map(
        per_device,
        mesh=mesh,
        in_specs=placed,
        out_specs=(token, token, token, token),
        check_vma=False,
    )
```

```python
import math

import jax
import jax.numpy as jnp
from jax import lax
from jax.experimental import pallas as pl
from jax.experimental.pallas import tpu as pltpu
from jax.sharding import PartitionSpec as P

KEY_VALUE_HEADS = 4
HEAD_SIZE = 128
EPSILON = 1e-06
BLOCK = 512
SHARES = (5, 3)
DELTA_ROWS = 16
DIGITS = 8


def dot_nn(left, right):
    return lax.dot_general(
        left, right, (((1,), (0,)), ((), ())), preferred_element_type=jnp.float32
    )


def contract_last(left, right):
    return lax.dot_general(
        left, right, (((1,), (1,)), ((), ())), preferred_element_type=jnp.float32
    )


def contract_first(left, right):
    return lax.dot_general(
        left, right, (((0,), (0,)), ((), ())), preferred_element_type=jnp.float32
    )


def project_kernel(resid_ref, weight_ref, output_ref, out_ref):
    parts, devices, heads, _, piece = weight_ref.shape
    head_width = heads * HEAD_SIZE
    total = None
    for part in range(parts):
        weight = weight_ref[part].reshape(devices * head_width, piece)
        term = contract_last(weight, resid_ref[:, part * piece : (part + 1) * piece])
        total = term if total is None else total + term
    row_at = lax.broadcasted_iota(jnp.int32, (DELTA_ROWS, resid_ref.shape[0]), 0)
    for device in range(devices):
        held = jnp.zeros(row_at.shape, jnp.float32)
        for head in range(heads):
            start = device * head_width + head * HEAD_SIZE
            grad = total[start : start + HEAD_SIZE].astype(jnp.bfloat16)
            output = output_ref[:, start : start + HEAD_SIZE].astype(jnp.float32).T
            rest = jnp.sum(grad.astype(jnp.float32) * output, axis=0, keepdims=True)
            for row in range(3):
                digit = rest.astype(jnp.bfloat16).astype(jnp.float32)
                held = jnp.where(row_at == DIGITS * head + row, digit, held)
                rest = rest - digit
            out_ref[device, head * HEAD_SIZE : (head + 1) * HEAD_SIZE] = grad
        out_ref[device, head_width:] = held.astype(jnp.bfloat16)


def project(resid, weights, attn_out):
    tokens, width = resid.shape
    parts, devices, heads, _, piece = weights.shape
    step = min(4, devices)
    out_rows = heads * HEAD_SIZE + DELTA_ROWS
    return pl.pallas_call(
        project_kernel,
        grid=(devices // step,),
        in_specs=[
            pl.BlockSpec((tokens, width), lambda n: (0, 0)),
            pl.BlockSpec((parts, step, heads, HEAD_SIZE, piece), lambda n: (0, n, 0, 0, 0)),
            pl.BlockSpec((tokens, step * heads * HEAD_SIZE), lambda n: (0, n)),
        ],
        out_specs=pl.BlockSpec((step, out_rows, tokens), lambda n: (n, 0, 0)),
        out_shape=jax.ShapeDtypeStruct((devices, out_rows, tokens), jnp.bfloat16),
        cost_estimate=pl.CostEstimate(
            flops=2 * tokens * width * devices * heads * HEAD_SIZE,
            bytes_accessed=2 * devices * heads * HEAD_SIZE * (width + 3 * tokens),
            transcendentals=0,
        ),
        name="project",
    )(resid, weights, attn_out)


def attention_kernel(packed_ref, grad_ref, lse_ref, out_ref, delta_ref, grad_t_ref, dqt_ref):
    j = pl.program_id(0)
    steps = pl.num_programs(0)
    heads = lse_ref.shape[0]
    length = packed_ref.shape[0]
    devices, _, tokens = grad_ref.shape
    block = min(BLOCK, length)
    scale = float(HEAD_SIZE) ** (-0.5)
    log2e = math.log2(math.e)
    key_from = heads * HEAD_SIZE
    value_from = key_from + HEAD_SIZE

    @pl.when(j == 0)
    def _():
        dqt_ref[...] = jnp.zeros_like(dqt_ref)
        for device in range(devices):
            cols = slice(device * tokens, (device + 1) * tokens)
            grad_t_ref[:, cols] = grad_ref[device, :key_from]
            digits = grad_ref[device, key_from:].astype(jnp.float32)
            for head in range(heads):
                rows = digits[DIGITS * head : DIGITS * (head + 1)]
                delta_ref[DIGITS * head : DIGITS * (head + 1), cols] = jnp.broadcast_to(
                    jnp.sum(rows, axis=0, keepdims=True), (DIGITS, tokens)
                )

    key_rows = pl.ds(pl.multiple_of(j * block, block), block)
    key = packed_ref[key_rows, key_from:value_from]
    value = packed_ref[key_rows, value_from : value_from + HEAD_SIZE]
    key_t = key.astype(jnp.float32).T.astype(jnp.bfloat16)

    def body(i, carry):
        dkey, dvalue = carry
        rows = pl.ds(pl.multiple_of(i * block, block), block)
        for head in range(heads):
            head_cols = slice(head * HEAD_SIZE, (head + 1) * HEAD_SIZE)
            query = packed_ref[rows, head_cols]
            grad_t = grad_t_ref[head_cols, rows]
            lse = lse_ref[head : head + 1, rows] * log2e
            delta = delta_ref[DIGITS * head : DIGITS * head + 1, rows]
            scores = contract_last(key, query)
            probs = jnp.exp2(scores * (scale * log2e) - lse)
            key_at = j * block + lax.broadcasted_iota(jnp.int32, scores.shape, 0)
            query_at = i * block + lax.broadcasted_iota(jnp.int32, scores.shape, 1)
            probs = jnp.where(key_at <= query_at, probs, 0.0)
            grad_probs = dot_nn(value, grad_t)
            grad_scores = (probs * (grad_probs - delta)).astype(jnp.bfloat16)
            dkey = dkey + dot_nn(grad_scores, query)
            dvalue = dvalue + contract_last(probs.astype(jnp.bfloat16), grad_t)
            dqt_ref[head_cols, rows] += dot_nn(key_t, grad_scores)
        return dkey, dvalue

    zero = jnp.zeros((block, HEAD_SIZE), jnp.float32)
    dkey, dvalue = lax.fori_loop(j, steps, body, (zero, zero))
    out_ref[key_rows, key_from:value_from] = (dkey * scale).astype(jnp.bfloat16)
    out_ref[key_rows, value_from:] = dvalue.astype(jnp.bfloat16)

    @pl.when(j == steps - 1)
    def _():
        for head in range(heads):
            head_cols = slice(head * HEAD_SIZE, (head + 1) * HEAD_SIZE)
            out_ref[:, head_cols] = (dqt_ref[head_cols, :].T * scale).astype(jnp.bfloat16)


def attention(packed, grad, lse):
    length, packed_width = packed.shape
    heads = lse.shape[0]
    block = min(BLOCK, length)

    def whole(shape):
        return pl.BlockSpec(shape, lambda j: (0,) * len(shape))

    return pl.pallas_call(
        attention_kernel,
        grid=(length // block,),
        in_specs=[whole(packed.shape), whole(grad.shape), whole(lse.shape)],
        out_specs=whole(packed.shape),
        out_shape=jax.ShapeDtypeStruct(packed.shape, jnp.bfloat16),
        scratch_shapes=[
            pltpu.VMEM((DIGITS * heads, length), jnp.float32),
            pltpu.VMEM((heads * HEAD_SIZE, length), jnp.bfloat16),
            pltpu.VMEM((heads * HEAD_SIZE, length), jnp.float32),
        ],
        compiler_params=pltpu.CompilerParams(
            dimension_semantics=("arbitrary",), vmem_limit_bytes=48 * 1024 * 1024
        ),
        cost_estimate=pl.CostEstimate(
            flops=10 * heads * length * length * HEAD_SIZE // 2,
            bytes_accessed=2 * length * (2 * packed_width + heads * HEAD_SIZE),
            transcendentals=heads * length * length // 2,
        ),
        name="attention",
    )(packed, grad, lse)


def assemble_kernel(packed_ref, query_ref, key_ref, value_ref):
    devices = packed_ref.shape[0]
    head_width = query_ref.shape[1] // devices
    total = packed_ref[0, :, head_width:].astype(jnp.float32)
    for device in range(1, devices):
        total = total + packed_ref[device, :, head_width:].astype(jnp.float32)
    key_ref[...] = total[:, :HEAD_SIZE].astype(jnp.bfloat16)
    value_ref[...] = total[:, HEAD_SIZE:].astype(jnp.bfloat16)
    for device in range(devices):
        cols = slice(device * head_width, (device + 1) * head_width)
        query_ref[:, cols] = packed_ref[device, :, :head_width]


def assemble(packed):
    devices, rows, packed_width = packed.shape
    shared = devices // KEY_VALUE_HEADS
    query_width = shared * (packed_width - 2 * HEAD_SIZE)
    widths = (query_width, HEAD_SIZE, HEAD_SIZE)
    return pl.pallas_call(
        assemble_kernel,
        grid=(KEY_VALUE_HEADS,),
        in_specs=[pl.BlockSpec((shared, rows, packed_width), lambda n: (n, 0, 0))],
        out_specs=[pl.BlockSpec((rows, width), lambda n: (0, n)) for width in widths],
        out_shape=[
            jax.ShapeDtypeStruct((rows, KEY_VALUE_HEADS * width), jnp.bfloat16)
            for width in widths
        ],
        name="assemble",
    )(packed)


def pick(array, index, axis):
    starts = [jnp.int32(0)] * array.ndim
    starts[axis] = index.astype(jnp.int32)
    sizes = list(array.shape)
    sizes[axis] = 1
    piece = lax.dynamic_slice(array, starts, sizes, allow_negative_indices=False)
    return lax.squeeze(piece, (axis,))


def scatter_sum(partial, groups, rows):
    grp_at = lax.axis_index("grp")
    core = lax.rem(grp_at, 2)
    place = lax.div(grp_at, 2)
    chips = groups // 2
    f32 = jnp.float32
    parts = partial.reshape(chips, 2, rows, partial.shape[1])
    keep = pick(parts, core, 1)
    send = pick(parts, 1 - core, 1)
    other = lax.ppermute(send, "grp", [(g, g ^ 1) for g in range(groups)])
    pair = (keep.astype(f32) + other.astype(f32)).astype(jnp.bfloat16)
    total = pick(pair, place, 0).astype(f32)
    for step in range(1, chips):
        block = pick(pair, lax.rem(place + step, chips), 0)
        moves = [(g, (g // 2 + step) % chips * 2 + g % 2) for g in range(groups)]
        block = lax.ppermute(block, "grp", moves)
        total = total + block.astype(f32)
    return total


def per_device(
    grad_out,
    hidden,
    norm_gain,
    expert_ids,
    gate_weights,
    w_gate,
    w_up,
    w_down,
    w_out,
    queries,
    keys,
    values,
    attn_out,
    lse,
):
    bf16, f32 = jnp.bfloat16, jnp.float32
    rows, width = hidden.shape
    topk = expert_ids.shape[1]
    groups = lax.axis_size("grp")
    inner = lax.axis_size("inner")
    grp_at = lax.axis_index("grp")
    experts = groups * inner
    capacity = max(2, 5 * rows * topk // (4 * experts))
    slots = groups * capacity
    column = groups * rows
    ff = w_gate.shape[2]
    head_width = queries.shape[1] // inner
    shared = inner // KEY_VALUE_HEADS

    hidden_f = hidden.astype(f32)
    inverse = lax.rsqrt(jnp.mean(hidden_f * hidden_f, axis=1, keepdims=True) + EPSILON)
    normed = (hidden_f * inverse * norm_gain).astype(bf16)

    normed_all = lax.all_gather(normed, "grp", axis=0, tiled=True)
    upstream_all = lax.all_gather(grad_out, "grp", axis=0, tiled=True)
    routing = jnp.concatenate([expert_ids.astype(f32).T, gate_weights.T], axis=0)
    routing = lax.all_gather(routing, "grp", axis=0, tiled=False)

    piece = width // groups
    w_piece = lax.dynamic_slice_in_dim(w_out, grp_at * piece, piece, axis=1)
    w_piece = jnp.broadcast_to(w_piece[None], (inner,) + w_piece.shape)
    w_piece = lax.all_to_all(w_piece, "inner", 0, 0, tiled=True)
    normed_all, w_piece = lax.optimization_barrier((normed_all, w_piece))
    w_whole = lax.all_gather(w_piece, "grp", axis=0, tiled=False)
    w_whole = w_whole.reshape(groups, inner, head_width // HEAD_SIZE, HEAD_SIZE, piece)

    ids_all = routing[:, :topk]
    gates_all = routing[:, topk:]
    mine = (grp_at * inner + lax.broadcasted_iota(jnp.int32, (1, inner, 1, 1), 1)).astype(f32)
    match = ids_all[:, None] == mine
    named = jnp.any(match, axis=2)
    gate = jnp.sum(jnp.where(match, gates_all[:, None], 0.0), axis=2)
    before = (
        lax.broadcasted_iota(jnp.int32, (rows, rows), 0)
        < lax.broadcasted_iota(jnp.int32, (rows, rows), 1)
    ).astype(bf16)
    rank = dot_nn(named.astype(bf16).reshape(groups * inner, rows), before)
    rank = rank.reshape(groups, inner, rows)
    block_at = lax.broadcasted_iota(jnp.int32, (groups, 1, 1), 0).astype(f32)
    slot = jnp.where(named, block_at * capacity + rank, -1.0)
    slot = slot.transpose(1, 0, 2).reshape(inner, 1, column)
    gate = gate.transpose(1, 0, 2).reshape(inner, 1, column)
    slot_at = lax.broadcasted_iota(jnp.int32, (1, slots, 1), 1).astype(f32)
    chosen = slot == slot_at
    picks = jnp.where(slot == slot_at, 1.0, 0.0).astype(bf16).reshape(inner * slots, column)
    picks = lax.optimization_barrier(picks)

    def to_experts(array):
        return lax.all_to_all(array, "inner", 0, 0, tiled=True).reshape(inner * slots, width)

    slot_gate = jnp.sum(jnp.where(chosen, gate, 0.0), axis=2)
    inputs = to_experts(dot_nn(picks, normed_all).astype(bf16).reshape(inner, slots, width))
    slot_gate = slot_gate.reshape(inner * slots, 1)
    upstream_rows = (dot_nn(picks, upstream_all) * slot_gate).astype(bf16)
    upstream_rows = to_experts(upstream_rows.reshape(inner, slots, width))

    kv = jnp.stack(
        [
            keys.reshape(rows, KEY_VALUE_HEADS, HEAD_SIZE),
            values.reshape(rows, KEY_VALUE_HEADS, HEAD_SIZE),
        ],
        axis=2,
    ).reshape(rows, KEY_VALUE_HEADS, 2 * HEAD_SIZE)
    kv = jnp.repeat(kv.transpose(1, 0, 2), shared, axis=0)
    packed = jnp.concatenate(
        [queries.reshape(rows, inner, head_width).transpose(1, 0, 2), kv], axis=2
    )

    w_gate_up = jnp.concatenate([w_gate[0], w_up[0]], axis=1)
    pre = dot_nn(inputs, w_gate_up)
    gate_pre = pre[:, :ff]
    up_pre = pre[:, ff:]
    sigmoid = jax.nn.sigmoid(gate_pre)
    gate_slope = (up_pre * sigmoid * (1.0 + gate_pre * (1.0 - sigmoid))).astype(bf16)
    up_slope = (gate_pre * sigmoid).astype(bf16)
    share = width // sum(SHARES)
    cuts = [share * sum(SHARES[:part]) for part in range(len(SHARES))] + [width]
    w_shares = [
        jnp.concatenate([w[0, low:high] for w in (w_gate, w_up)], axis=1)
        for low, high in zip(cuts[:-1], cuts[1:])
    ]
    upstream_rows, w_whole, packed, gate_slope, up_slope, w_shares = lax.optimization_barrier(
        (upstream_rows, w_whole, packed, gate_slope, up_slope, w_shares)
    )
    back_hidden = contract_last(upstream_rows, w_down[0])
    grad_gate = (back_hidden * gate_slope).astype(bf16)
    grad_up = (back_hidden * up_slope).astype(bf16)
    grad_both = jnp.concatenate([grad_gate, grad_up], axis=1)

    def add_up(rows_back):
        rows_back = rows_back.reshape(inner * slots, rows_back.shape[2])
        return contract_first(picks, rows_back).astype(bf16)

    sums = []
    grads = []
    for part in range(len(SHARES)):
        grads.append(contract_last(grad_both, w_shares[part]))
        grads[part] = grads[part].astype(bf16).reshape(inner, slots, -1)
    for part in range(len(SHARES)):
        if part > 0:
            returned, grads[part] = lax.optimization_barrier((returned, grads[part]))
        arrived = lax.all_to_all(grads[part], "inner", 0, 0, tiled=True)
        if part > 0:
            sums.append(scatter_sum(add_up(returned), groups, rows))
        returned = arrived
    packed, returned = lax.optimization_barrier((packed, returned))
    packed = lax.all_to_all(packed, "inner", 0, 0, tiled=True)
    packed = packed.reshape(inner * rows, head_width + 2 * HEAD_SIZE)
    sums.append(scatter_sum(add_up(returned), groups, rows))
    grad_normed = jnp.concatenate(sums, axis=1)

    gained = grad_normed * norm_gain
    statistic = jnp.mean(gained * hidden_f, axis=1, keepdims=True)
    grad_resid = (
        grad_out.astype(f32)
        + inverse * gained
        - hidden_f * inverse * inverse * inverse * statistic
    ).astype(bf16)

    head_grad = project(grad_resid, w_whole, attn_out)
    head_grad, packed = lax.optimization_barrier((head_grad, packed))
    head_grad = lax.all_to_all(head_grad, "inner", 0, 0, tiled=True)
    packed_grads = attention(packed, head_grad, lse)
    packed_grads = packed_grads.reshape(inner, rows, head_width + 2 * HEAD_SIZE)
    packed_grads = lax.all_to_all(packed_grads, "inner", 0, 0, tiled=True)
    queries_gradient, keys_gradient, values_gradient = assemble(packed_grads)
    return (grad_resid, queries_gradient, keys_gradient, values_gradient)


def solution(mesh):
    token = P(("grp", "inner"), None)
    expert = P(("grp", "inner"), None, None)
    placed = (
        token,
        token,
        P(),
        token,
        token,
        expert,
        expert,
        expert,
        P("inner", None),
        token,
        token,
        token,
        token,
        P("inner", "grp"),
    )

    return jax.shard_map(
        per_device,
        mesh=mesh,
        in_specs=placed,
        out_specs=(token, token, token, token),
        check_vma=False,
    )
```

```python
import math

import jax
import jax.numpy as jnp
from jax import lax
from jax.experimental import pallas as pl
from jax.experimental.pallas import tpu as pltpu
from jax.sharding import PartitionSpec as P

KEY_VALUE_HEADS = 4
HEAD_SIZE = 128
EPSILON = 1e-06
BLOCK = 512
SHARES = (5, 3)
DELTA_ROWS = 16
DIGITS = 8


def dot_nn(left, right):
    return lax.dot_general(
        left, right, (((1,), (0,)), ((), ())), preferred_element_type=jnp.float32
    )


def contract_last(left, right):
    return lax.dot_general(
        left, right, (((1,), (1,)), ((), ())), preferred_element_type=jnp.float32
    )


def contract_first(left, right):
    return lax.dot_general(
        left, right, (((0,), (0,)), ((), ())), preferred_element_type=jnp.float32
    )


def project_kernel(resid_ref, weight_ref, output_ref, out_ref):
    parts, devices, heads, _, piece = weight_ref.shape
    head_width = heads * HEAD_SIZE
    total = None
    for part in range(parts):
        weight = weight_ref[part].reshape(devices * head_width, piece)
        term = contract_last(weight, resid_ref[:, part * piece : (part + 1) * piece])
        total = term if total is None else total + term
    row_at = lax.broadcasted_iota(jnp.int32, (DELTA_ROWS, resid_ref.shape[0]), 0)
    for device in range(devices):
        held = jnp.zeros(row_at.shape, jnp.float32)
        for head in range(heads):
            start = device * head_width + head * HEAD_SIZE
            grad = total[start : start + HEAD_SIZE].astype(jnp.bfloat16)
            output = output_ref[:, start : start + HEAD_SIZE].astype(jnp.float32).T
            rest = jnp.sum(grad.astype(jnp.float32) * output, axis=0, keepdims=True)
            for row in range(3):
                digit = rest.astype(jnp.bfloat16).astype(jnp.float32)
                held = jnp.where(row_at == DIGITS * head + row, digit, held)
                rest = rest - digit
            out_ref[device, head * HEAD_SIZE : (head + 1) * HEAD_SIZE] = grad
        out_ref[device, head_width:] = held.astype(jnp.bfloat16)


def project(resid, weights, attn_out):
    tokens, width = resid.shape
    parts, devices, heads, _, piece = weights.shape
    step = min(4, devices)
    out_rows = heads * HEAD_SIZE + DELTA_ROWS
    return pl.pallas_call(
        project_kernel,
        grid=(devices // step,),
        in_specs=[
            pl.BlockSpec((tokens, width), lambda n: (0, 0)),
            pl.BlockSpec((parts, step, heads, HEAD_SIZE, piece), lambda n: (0, n, 0, 0, 0)),
            pl.BlockSpec((tokens, step * heads * HEAD_SIZE), lambda n: (0, n)),
        ],
        out_specs=pl.BlockSpec((step, out_rows, tokens), lambda n: (n, 0, 0)),
        out_shape=jax.ShapeDtypeStruct((devices, out_rows, tokens), jnp.bfloat16),
        cost_estimate=pl.CostEstimate(
            flops=2 * tokens * width * devices * heads * HEAD_SIZE,
            bytes_accessed=2 * devices * heads * HEAD_SIZE * (width + 3 * tokens),
            transcendentals=0,
        ),
        name="project",
    )(resid, weights, attn_out)


def attention_kernel(packed_ref, grad_ref, lse_ref, out_ref, delta_ref, grad_t_ref, dqt_ref):
    j = pl.program_id(0)
    steps = pl.num_programs(0)
    heads = lse_ref.shape[0]
    length = packed_ref.shape[0]
    devices, _, tokens = grad_ref.shape
    block = min(BLOCK, length)
    scale = float(HEAD_SIZE) ** (-0.5)
    log2e = math.log2(math.e)
    key_from = heads * HEAD_SIZE
    value_from = key_from + HEAD_SIZE

    @pl.when(j == 0)
    def _():
        dqt_ref[...] = jnp.zeros_like(dqt_ref)
        for device in range(devices):
            cols = slice(device * tokens, (device + 1) * tokens)
            grad_t_ref[:, cols] = grad_ref[device, :key_from]
            digits = grad_ref[device, key_from:].astype(jnp.float32)
            for head in range(heads):
                rows = digits[DIGITS * head : DIGITS * (head + 1)]
                delta_ref[DIGITS * head : DIGITS * (head + 1), cols] = jnp.broadcast_to(
                    jnp.sum(rows, axis=0, keepdims=True), (DIGITS, tokens)
                )

    key_rows = pl.ds(pl.multiple_of(j * block, block), block)
    key = packed_ref[key_rows, key_from:value_from]
    value = packed_ref[key_rows, value_from : value_from + HEAD_SIZE]
    key_t = key.astype(jnp.float32).T.astype(jnp.bfloat16)

    def body(i, carry):
        dkey, dvalue = carry
        rows = pl.ds(pl.multiple_of(i * block, block), block)
        for head in range(heads):
            head_cols = slice(head * HEAD_SIZE, (head + 1) * HEAD_SIZE)
            query = packed_ref[rows, head_cols]
            grad_t = grad_t_ref[head_cols, rows]
            lse = lse_ref[head : head + 1, rows] * log2e
            delta = delta_ref[DIGITS * head : DIGITS * head + 1, rows]
            scores = contract_last(key, query)
            probs = jnp.exp2(scores * (scale * log2e) - lse)
            key_at = j * block + lax.broadcasted_iota(jnp.int32, scores.shape, 0)
            query_at = i * block + lax.broadcasted_iota(jnp.int32, scores.shape, 1)
            probs = jnp.where(key_at <= query_at, probs, 0.0)
            grad_probs = dot_nn(value, grad_t)
            grad_scores = (probs * (grad_probs - delta)).astype(jnp.bfloat16)
            dkey = dkey + dot_nn(grad_scores, query)
            dvalue = dvalue + contract_last(probs.astype(jnp.bfloat16), grad_t)
            dqt_ref[head_cols, rows] += dot_nn(key_t, grad_scores)
        return dkey, dvalue

    zero = jnp.zeros((block, HEAD_SIZE), jnp.float32)
    dkey, dvalue = lax.fori_loop(j, steps, body, (zero, zero))
    out_ref[key_rows, key_from:value_from] = (dkey * scale).astype(jnp.bfloat16)
    out_ref[key_rows, value_from:] = dvalue.astype(jnp.bfloat16)

    @pl.when(j == steps - 1)
    def _():
        for head in range(heads):
            head_cols = slice(head * HEAD_SIZE, (head + 1) * HEAD_SIZE)
            out_ref[:, head_cols] = (dqt_ref[head_cols, :].T * scale).astype(jnp.bfloat16)


def attention(packed, grad, lse):
    length, packed_width = packed.shape
    heads = lse.shape[0]
    block = min(BLOCK, length)

    def whole(shape):
        return pl.BlockSpec(shape, lambda j: (0,) * len(shape))

    return pl.pallas_call(
        attention_kernel,
        grid=(length // block,),
        in_specs=[whole(packed.shape), whole(grad.shape), whole(lse.shape)],
        out_specs=whole(packed.shape),
        out_shape=jax.ShapeDtypeStruct(packed.shape, jnp.bfloat16),
        scratch_shapes=[
            pltpu.VMEM((DIGITS * heads, length), jnp.float32),
            pltpu.VMEM((heads * HEAD_SIZE, length), jnp.bfloat16),
            pltpu.VMEM((heads * HEAD_SIZE, length), jnp.float32),
        ],
        compiler_params=pltpu.CompilerParams(
            dimension_semantics=("arbitrary",), vmem_limit_bytes=48 * 1024 * 1024
        ),
        cost_estimate=pl.CostEstimate(
            flops=10 * heads * length * length * HEAD_SIZE // 2,
            bytes_accessed=2 * length * (2 * packed_width + heads * HEAD_SIZE),
            transcendentals=heads * length * length // 2,
        ),
        name="attention",
    )(packed, grad, lse)


def assemble_kernel(packed_ref, query_ref, key_ref, value_ref):
    devices = packed_ref.shape[0]
    head_width = query_ref.shape[1] // devices
    total = packed_ref[0, :, head_width:].astype(jnp.float32)
    for device in range(1, devices):
        total = total + packed_ref[device, :, head_width:].astype(jnp.float32)
    key_ref[...] = total[:, :HEAD_SIZE].astype(jnp.bfloat16)
    value_ref[...] = total[:, HEAD_SIZE:].astype(jnp.bfloat16)
    for device in range(devices):
        cols = slice(device * head_width, (device + 1) * head_width)
        query_ref[:, cols] = packed_ref[device, :, :head_width]


def assemble(packed):
    devices, rows, packed_width = packed.shape
    shared = devices // KEY_VALUE_HEADS
    query_width = shared * (packed_width - 2 * HEAD_SIZE)
    widths = (query_width, HEAD_SIZE, HEAD_SIZE)
    return pl.pallas_call(
        assemble_kernel,
        grid=(KEY_VALUE_HEADS,),
        in_specs=[pl.BlockSpec((shared, rows, packed_width), lambda n: (n, 0, 0))],
        out_specs=[pl.BlockSpec((rows, width), lambda n: (0, n)) for width in widths],
        out_shape=[
            jax.ShapeDtypeStruct((rows, KEY_VALUE_HEADS * width), jnp.bfloat16)
            for width in widths
        ],
        name="assemble",
    )(packed)


def pick(array, index, axis):
    starts = [jnp.int32(0)] * array.ndim
    starts[axis] = index.astype(jnp.int32)
    sizes = list(array.shape)
    sizes[axis] = 1
    piece = lax.dynamic_slice(array, starts, sizes, allow_negative_indices=False)
    return lax.squeeze(piece, (axis,))


def scatter_sum(partial, groups, rows):
    grp_at = lax.axis_index("grp")
    core = lax.rem(grp_at, 2)
    place = lax.div(grp_at, 2)
    chips = groups // 2
    f32 = jnp.float32
    parts = partial.reshape(chips, 2, rows, partial.shape[1])
    keep = pick(parts, core, 1)
    send = pick(parts, 1 - core, 1)
    other = lax.ppermute(send, "grp", [(g, g ^ 1) for g in range(groups)])
    pair = (keep.astype(f32) + other.astype(f32)).astype(jnp.bfloat16)
    total = pick(pair, place, 0).astype(f32)
    for step in range(1, chips):
        block = pick(pair, lax.rem(place + step, chips), 0)
        moves = [(g, (g // 2 + step) % chips * 2 + g % 2) for g in range(groups)]
        block = lax.ppermute(block, "grp", moves)
        total = total + block.astype(f32)
    return total


def per_device(
    grad_out,
    hidden,
    norm_gain,
    expert_ids,
    gate_weights,
    w_gate,
    w_up,
    w_down,
    w_out,
    queries,
    keys,
    values,
    attn_out,
    lse,
):
    bf16, f32 = jnp.bfloat16, jnp.float32
    rows, width = hidden.shape
    topk = expert_ids.shape[1]
    groups = lax.axis_size("grp")
    inner = lax.axis_size("inner")
    grp_at = lax.axis_index("grp")
    experts = groups * inner
    capacity = max(2, 5 * rows * topk // (4 * experts))
    slots = groups * capacity
    column = groups * rows
    ff = w_gate.shape[2]
    head_width = queries.shape[1] // inner
    shared = inner // KEY_VALUE_HEADS

    hidden_f = hidden.astype(f32)
    inverse = lax.rsqrt(jnp.mean(hidden_f * hidden_f, axis=1, keepdims=True) + EPSILON)
    normed = (hidden_f * inverse * norm_gain).astype(bf16)

    normed_all = lax.all_gather(normed, "grp", axis=0, tiled=True)
    upstream_all = lax.all_gather(grad_out, "grp", axis=0, tiled=True)
    routing = jnp.concatenate([expert_ids.astype(f32).T, gate_weights.T], axis=0)
    routing = lax.all_gather(routing, "grp", axis=0, tiled=False)

    piece = width // groups
    w_piece = lax.dynamic_slice_in_dim(w_out, grp_at * piece, piece, axis=1)
    w_piece = jnp.broadcast_to(w_piece[None], (inner,) + w_piece.shape)
    w_piece = lax.all_to_all(w_piece, "inner", 0, 0, tiled=True)
    ids_all = routing[:, :topk]
    gates_all = routing[:, topk:]
    mine = (grp_at * inner + lax.broadcasted_iota(jnp.int32, (1, inner, 1, 1), 1)).astype(f32)
    match = ids_all[:, None] == mine
    named = jnp.any(match, axis=2)
    gate = jnp.sum(jnp.where(match, gates_all[:, None], 0.0), axis=2)
    before = (
        lax.broadcasted_iota(jnp.int32, (rows, rows), 0)
        < lax.broadcasted_iota(jnp.int32, (rows, rows), 1)
    ).astype(bf16)
    rank = dot_nn(named.astype(bf16).reshape(groups * inner, rows), before)
    rank = rank.reshape(groups, inner, rows)
    block_at = lax.broadcasted_iota(jnp.int32, (groups, 1, 1), 0).astype(f32)
    slot = jnp.where(named, block_at * capacity + rank, -1.0)
    slot = slot.transpose(1, 0, 2).reshape(inner, 1, column)
    gate = gate.transpose(1, 0, 2).reshape(inner, 1, column)
    slot_at = lax.broadcasted_iota(jnp.int32, (1, slots, 1), 1).astype(f32)
    chosen = slot == slot_at
    picks = jnp.where(slot == slot_at, 1.0, 0.0).astype(bf16).reshape(inner * slots, column)
    picks = lax.optimization_barrier(picks)

    def to_experts(array):
        return lax.all_to_all(array, "inner", 0, 0, tiled=True).reshape(inner * slots, width)

    slot_gate = jnp.sum(jnp.where(chosen, gate, 0.0), axis=2)
    input_rows = dot_nn(picks, normed_all).astype(bf16)
    input_rows, w_piece = lax.optimization_barrier((input_rows, w_piece))
    w_whole = lax.all_gather(w_piece, "grp", axis=0, tiled=False)
    w_whole = w_whole.reshape(groups, inner, head_width // HEAD_SIZE, HEAD_SIZE, piece)
    inputs = to_experts(input_rows.reshape(inner, slots, width))
    slot_gate = slot_gate.reshape(inner * slots, 1)
    upstream_rows = (dot_nn(picks, upstream_all) * slot_gate).astype(bf16)
    upstream_rows = to_experts(upstream_rows.reshape(inner, slots, width))

    kv = jnp.stack(
        [
            keys.reshape(rows, KEY_VALUE_HEADS, HEAD_SIZE),
            values.reshape(rows, KEY_VALUE_HEADS, HEAD_SIZE),
        ],
        axis=2,
    ).reshape(rows, KEY_VALUE_HEADS, 2 * HEAD_SIZE)
    kv = jnp.repeat(kv.transpose(1, 0, 2), shared, axis=0)
    packed = jnp.concatenate(
        [queries.reshape(rows, inner, head_width).transpose(1, 0, 2), kv], axis=2
    )

    w_gate_up = jnp.concatenate([w_gate[0], w_up[0]], axis=1)
    pre = dot_nn(inputs, w_gate_up)
    gate_pre = pre[:, :ff]
    up_pre = pre[:, ff:]
    sigmoid = jax.nn.sigmoid(gate_pre)
    gate_slope = (up_pre * sigmoid * (1.0 + gate_pre * (1.0 - sigmoid))).astype(bf16)
    up_slope = (gate_pre * sigmoid).astype(bf16)
    share = width // sum(SHARES)
    cuts = [share * sum(SHARES[:part]) for part in range(len(SHARES))] + [width]
    w_shares = [
        jnp.concatenate([w[0, low:high] for w in (w_gate, w_up)], axis=1)
        for low, high in zip(cuts[:-1], cuts[1:])
    ]
    upstream_rows, w_whole, packed, gate_slope, up_slope, w_shares = lax.optimization_barrier(
        (upstream_rows, w_whole, packed, gate_slope, up_slope, w_shares)
    )
    back_hidden = contract_last(upstream_rows, w_down[0])
    grad_gate = (back_hidden * gate_slope).astype(bf16)
    grad_up = (back_hidden * up_slope).astype(bf16)
    grad_both = jnp.concatenate([grad_gate, grad_up], axis=1)

    def add_up(rows_back):
        rows_back = rows_back.reshape(inner * slots, rows_back.shape[2])
        return contract_first(picks, rows_back).astype(bf16)

    sums = []
    grads = []
    for part in range(len(SHARES)):
        grads.append(contract_last(grad_both, w_shares[part]))
        grads[part] = grads[part].astype(bf16).reshape(inner, slots, -1)
    for part in range(len(SHARES)):
        if part > 0:
            returned, grads[part] = lax.optimization_barrier((returned, grads[part]))
        arrived = lax.all_to_all(grads[part], "inner", 0, 0, tiled=True)
        if part > 0:
            sums.append(scatter_sum(add_up(returned), groups, rows))
        returned = arrived
    packed, returned = lax.optimization_barrier((packed, returned))
    packed = lax.all_to_all(packed, "inner", 0, 0, tiled=True)
    packed = packed.reshape(inner * rows, head_width + 2 * HEAD_SIZE)
    sums.append(scatter_sum(add_up(returned), groups, rows))
    grad_normed = jnp.concatenate(sums, axis=1)

    gained = grad_normed * norm_gain
    statistic = jnp.mean(gained * hidden_f, axis=1, keepdims=True)
    grad_resid = (
        grad_out.astype(f32)
        + inverse * gained
        - hidden_f * inverse * inverse * inverse * statistic
    ).astype(bf16)

    head_grad = project(grad_resid, w_whole, attn_out)
    head_grad, packed = lax.optimization_barrier((head_grad, packed))
    head_grad = lax.all_to_all(head_grad, "inner", 0, 0, tiled=True)
    packed_grads = attention(packed, head_grad, lse)
    packed_grads = packed_grads.reshape(inner, rows, head_width + 2 * HEAD_SIZE)
    packed_grads = lax.all_to_all(packed_grads, "inner", 0, 0, tiled=True)
    queries_gradient, keys_gradient, values_gradient = assemble(packed_grads)
    return (grad_resid, queries_gradient, keys_gradient, values_gradient)


def solution(mesh):
    token = P(("grp", "inner"), None)
    expert = P(("grp", "inner"), None, None)
    placed = (
        token,
        token,
        P(),
        token,
        token,
        expert,
        expert,
        expert,
        P("inner", None),
        token,
        token,
        token,
        token,
        P("inner", "grp"),
    )

    return jax.shard_map(
        per_device,
        mesh=mesh,
        in_specs=placed,
        out_specs=(token, token, token, token),
        check_vma=False,
    )
```

```python
import math

import jax
import jax.numpy as jnp
from jax import lax
from jax.experimental import pallas as pl
from jax.experimental.pallas import tpu as pltpu
from jax.sharding import PartitionSpec as P

KEY_VALUE_HEADS = 4
HEAD_SIZE = 128
EPSILON = 1e-06
BLOCK = 512
SHARES = (5, 3)
DELTA_ROWS = 16
DIGITS = 8


def dot_nn(left, right):
    return lax.dot_general(
        left, right, (((1,), (0,)), ((), ())), preferred_element_type=jnp.float32
    )


def contract_last(left, right):
    return lax.dot_general(
        left, right, (((1,), (1,)), ((), ())), preferred_element_type=jnp.float32
    )


def contract_first(left, right):
    return lax.dot_general(
        left, right, (((0,), (0,)), ((), ())), preferred_element_type=jnp.float32
    )


def project_kernel(resid_ref, weight_ref, output_ref, out_ref):
    parts, devices, heads, _, piece = weight_ref.shape
    head_width = heads * HEAD_SIZE
    total = None
    for part in range(parts):
        weight = weight_ref[part].reshape(devices * head_width, piece)
        term = contract_last(weight, resid_ref[:, part * piece : (part + 1) * piece])
        total = term if total is None else total + term
    row_at = lax.broadcasted_iota(jnp.int32, (DELTA_ROWS, resid_ref.shape[0]), 0)
    for device in range(devices):
        held = jnp.zeros(row_at.shape, jnp.float32)
        for head in range(heads):
            start = device * head_width + head * HEAD_SIZE
            grad = total[start : start + HEAD_SIZE].astype(jnp.bfloat16)
            output = output_ref[:, start : start + HEAD_SIZE].astype(jnp.float32).T
            rest = jnp.sum(grad.astype(jnp.float32) * output, axis=0, keepdims=True)
            for row in range(3):
                digit = rest.astype(jnp.bfloat16).astype(jnp.float32)
                held = jnp.where(row_at == DIGITS * head + row, digit, held)
                rest = rest - digit
            out_ref[device, head * HEAD_SIZE : (head + 1) * HEAD_SIZE] = grad
        out_ref[device, head_width:] = held.astype(jnp.bfloat16)


def project(resid, weights, attn_out):
    tokens, width = resid.shape
    parts, devices, heads, _, piece = weights.shape
    step = min(4, devices)
    out_rows = heads * HEAD_SIZE + DELTA_ROWS
    return pl.pallas_call(
        project_kernel,
        grid=(devices // step,),
        in_specs=[
            pl.BlockSpec((tokens, width), lambda n: (0, 0)),
            pl.BlockSpec((parts, step, heads, HEAD_SIZE, piece), lambda n: (0, n, 0, 0, 0)),
            pl.BlockSpec((tokens, step * heads * HEAD_SIZE), lambda n: (0, n)),
        ],
        out_specs=pl.BlockSpec((step, out_rows, tokens), lambda n: (n, 0, 0)),
        out_shape=jax.ShapeDtypeStruct((devices, out_rows, tokens), jnp.bfloat16),
        cost_estimate=pl.CostEstimate(
            flops=2 * tokens * width * devices * heads * HEAD_SIZE,
            bytes_accessed=2 * devices * heads * HEAD_SIZE * (width + 3 * tokens),
            transcendentals=0,
        ),
        name="project",
    )(resid, weights, attn_out)


def attention_kernel(packed_ref, grad_ref, lse_ref, out_ref, delta_ref, grad_t_ref, dqt_ref):
    j = pl.program_id(0)
    steps = pl.num_programs(0)
    heads = lse_ref.shape[0]
    length = packed_ref.shape[0]
    devices, _, tokens = grad_ref.shape
    block = min(BLOCK, length)
    scale = float(HEAD_SIZE) ** (-0.5)
    log2e = math.log2(math.e)
    key_from = heads * HEAD_SIZE
    value_from = key_from + HEAD_SIZE

    @pl.when(j == 0)
    def _():
        dqt_ref[...] = jnp.zeros_like(dqt_ref)
        for device in range(devices):
            cols = slice(device * tokens, (device + 1) * tokens)
            grad_t_ref[:, cols] = grad_ref[device, :key_from]
            digits = grad_ref[device, key_from:].astype(jnp.float32)
            for head in range(heads):
                rows = digits[DIGITS * head : DIGITS * (head + 1)]
                delta_ref[DIGITS * head : DIGITS * (head + 1), cols] = jnp.broadcast_to(
                    jnp.sum(rows, axis=0, keepdims=True), (DIGITS, tokens)
                )

    key_rows = pl.ds(pl.multiple_of(j * block, block), block)
    key = packed_ref[key_rows, key_from:value_from]
    value = packed_ref[key_rows, value_from : value_from + HEAD_SIZE]
    key_t = key.astype(jnp.float32).T.astype(jnp.bfloat16)

    def body(i, carry):
        dkey, dvalue = carry
        rows = pl.ds(pl.multiple_of(i * block, block), block)
        for head in range(heads):
            head_cols = slice(head * HEAD_SIZE, (head + 1) * HEAD_SIZE)
            query = packed_ref[rows, head_cols]
            grad_t = grad_t_ref[head_cols, rows]
            lse = lse_ref[head : head + 1, rows] * log2e
            delta = delta_ref[DIGITS * head : DIGITS * head + 1, rows]
            scores = contract_last(key, query)
            probs = jnp.exp2(scores * (scale * log2e) - lse)
            key_at = j * block + lax.broadcasted_iota(jnp.int32, scores.shape, 0)
            query_at = i * block + lax.broadcasted_iota(jnp.int32, scores.shape, 1)
            probs = jnp.where(key_at <= query_at, probs, 0.0)
            grad_probs = dot_nn(value, grad_t)
            grad_scores = (probs * (grad_probs - delta)).astype(jnp.bfloat16)
            dkey = dkey + dot_nn(grad_scores, query)
            dvalue = dvalue + contract_last(probs.astype(jnp.bfloat16), grad_t)
            dqt_ref[head_cols, rows] += dot_nn(key_t, grad_scores)
        return dkey, dvalue

    zero = jnp.zeros((block, HEAD_SIZE), jnp.float32)
    dkey, dvalue = lax.fori_loop(j, steps, body, (zero, zero))
    out_ref[key_rows, key_from:value_from] = (dkey * scale).astype(jnp.bfloat16)
    out_ref[key_rows, value_from:] = dvalue.astype(jnp.bfloat16)

    @pl.when(j == steps - 1)
    def _():
        for head in range(heads):
            head_cols = slice(head * HEAD_SIZE, (head + 1) * HEAD_SIZE)
            out_ref[:, head_cols] = (dqt_ref[head_cols, :].T * scale).astype(jnp.bfloat16)


def attention(packed, grad, lse):
    length, packed_width = packed.shape
    heads = lse.shape[0]
    block = min(BLOCK, length)

    def whole(shape):
        return pl.BlockSpec(shape, lambda j: (0,) * len(shape))

    return pl.pallas_call(
        attention_kernel,
        grid=(length // block,),
        in_specs=[whole(packed.shape), whole(grad.shape), whole(lse.shape)],
        out_specs=whole(packed.shape),
        out_shape=jax.ShapeDtypeStruct(packed.shape, jnp.bfloat16),
        scratch_shapes=[
            pltpu.VMEM((DIGITS * heads, length), jnp.float32),
            pltpu.VMEM((heads * HEAD_SIZE, length), jnp.bfloat16),
            pltpu.VMEM((heads * HEAD_SIZE, length), jnp.float32),
        ],
        compiler_params=pltpu.CompilerParams(
            dimension_semantics=("arbitrary",), vmem_limit_bytes=48 * 1024 * 1024
        ),
        cost_estimate=pl.CostEstimate(
            flops=10 * heads * length * length * HEAD_SIZE // 2,
            bytes_accessed=2 * length * (2 * packed_width + heads * HEAD_SIZE),
            transcendentals=heads * length * length // 2,
        ),
        name="attention",
    )(packed, grad, lse)


def assemble_kernel(packed_ref, query_ref, key_ref, value_ref):
    devices = packed_ref.shape[0]
    head_width = query_ref.shape[1] // devices
    total = packed_ref[0, :, head_width:].astype(jnp.float32)
    for device in range(1, devices):
        total = total + packed_ref[device, :, head_width:].astype(jnp.float32)
    key_ref[...] = total[:, :HEAD_SIZE].astype(jnp.bfloat16)
    value_ref[...] = total[:, HEAD_SIZE:].astype(jnp.bfloat16)
    for device in range(devices):
        cols = slice(device * head_width, (device + 1) * head_width)
        query_ref[:, cols] = packed_ref[device, :, :head_width]


def assemble(packed):
    devices, rows, packed_width = packed.shape
    shared = devices // KEY_VALUE_HEADS
    query_width = shared * (packed_width - 2 * HEAD_SIZE)
    widths = (query_width, HEAD_SIZE, HEAD_SIZE)
    return pl.pallas_call(
        assemble_kernel,
        grid=(KEY_VALUE_HEADS,),
        in_specs=[pl.BlockSpec((shared, rows, packed_width), lambda n: (n, 0, 0))],
        out_specs=[pl.BlockSpec((rows, width), lambda n: (0, n)) for width in widths],
        out_shape=[
            jax.ShapeDtypeStruct((rows, KEY_VALUE_HEADS * width), jnp.bfloat16)
            for width in widths
        ],
        name="assemble",
    )(packed)


def pick(array, index, axis):
    starts = [jnp.int32(0)] * array.ndim
    starts[axis] = index.astype(jnp.int32)
    sizes = list(array.shape)
    sizes[axis] = 1
    piece = lax.dynamic_slice(array, starts, sizes, allow_negative_indices=False)
    return lax.squeeze(piece, (axis,))


def scatter_sum(partial, groups, rows):
    grp_at = lax.axis_index("grp")
    core = lax.rem(grp_at, 2)
    place = lax.div(grp_at, 2)
    chips = groups // 2
    f32 = jnp.float32
    parts = partial.reshape(chips, 2, rows, partial.shape[1])
    keep = pick(parts, core, 1)
    send = pick(parts, 1 - core, 1)
    other = lax.ppermute(send, "grp", [(g, g ^ 1) for g in range(groups)])
    pair = (keep.astype(f32) + other.astype(f32)).astype(jnp.bfloat16)
    total = pick(pair, place, 0).astype(f32)
    for step in range(1, chips):
        block = pick(pair, lax.rem(place + step, chips), 0)
        moves = [(g, (g // 2 + step) % chips * 2 + g % 2) for g in range(groups)]
        block = lax.ppermute(block, "grp", moves)
        total = total + block.astype(f32)
    return total


def per_device(
    grad_out,
    hidden,
    norm_gain,
    expert_ids,
    gate_weights,
    w_gate,
    w_up,
    w_down,
    w_out,
    queries,
    keys,
    values,
    attn_out,
    lse,
):
    bf16, f32 = jnp.bfloat16, jnp.float32
    rows, width = hidden.shape
    topk = expert_ids.shape[1]
    groups = lax.axis_size("grp")
    inner = lax.axis_size("inner")
    grp_at = lax.axis_index("grp")
    experts = groups * inner
    capacity = max(2, 5 * rows * topk // (4 * experts))
    slots = groups * capacity
    column = groups * rows
    ff = w_gate.shape[2]
    head_width = queries.shape[1] // inner
    shared = inner // KEY_VALUE_HEADS

    hidden_f = hidden.astype(f32)
    inverse = lax.rsqrt(jnp.mean(hidden_f * hidden_f, axis=1, keepdims=True) + EPSILON)
    normed = (hidden_f * inverse * norm_gain).astype(bf16)

    normed_all = lax.all_gather(normed, "grp", axis=0, tiled=True)
    upstream_all = lax.all_gather(grad_out, "grp", axis=0, tiled=True)
    routing = jnp.concatenate([expert_ids.astype(f32).T, gate_weights.T], axis=0)
    routing = lax.all_gather(routing, "grp", axis=0, tiled=False)

    piece = width // groups
    w_piece = lax.dynamic_slice_in_dim(w_out, grp_at * piece, piece, axis=1)
    w_piece = jnp.broadcast_to(w_piece[None], (inner,) + w_piece.shape)
    w_piece = lax.all_to_all(w_piece, "inner", 0, 0, tiled=True)
    ids_all = routing[:, :topk]
    gates_all = routing[:, topk:]
    mine = (grp_at * inner + lax.broadcasted_iota(jnp.int32, (1, inner, 1, 1), 1)).astype(f32)
    match = ids_all[:, None] == mine
    named = jnp.any(match, axis=2)
    gate = jnp.sum(jnp.where(match, gates_all[:, None], 0.0), axis=2)
    before = (
        lax.broadcasted_iota(jnp.int32, (rows, rows), 0)
        < lax.broadcasted_iota(jnp.int32, (rows, rows), 1)
    ).astype(bf16)
    rank = dot_nn(named.astype(bf16).reshape(groups * inner, rows), before)
    rank = rank.reshape(groups, inner, rows)
    block_at = lax.broadcasted_iota(jnp.int32, (groups, 1, 1), 0).astype(f32)
    slot = jnp.where(named, block_at * capacity + rank, -1.0)
    slot = slot.transpose(1, 0, 2).reshape(inner, 1, column)
    gate = gate.transpose(1, 0, 2).reshape(inner, 1, column)
    slot_at = lax.broadcasted_iota(jnp.int32, (1, slots, 1), 1).astype(f32)
    chosen = slot == slot_at
    picks = jnp.where(slot == slot_at, 1.0, 0.0).astype(bf16).reshape(inner * slots, column)
    picks = lax.optimization_barrier(picks)

    def to_experts(array):
        return lax.all_to_all(array, "inner", 0, 0, tiled=True).reshape(inner * slots, width)

    slot_gate = jnp.sum(jnp.where(chosen, gate, 0.0), axis=2)
    input_rows = dot_nn(picks, normed_all).astype(bf16)
    input_rows, w_piece, slot_gate = lax.optimization_barrier((input_rows, w_piece, slot_gate))
    w_whole = lax.all_gather(w_piece, "grp", axis=0, tiled=False)
    w_whole = w_whole.reshape(groups, inner, head_width // HEAD_SIZE, HEAD_SIZE, piece)
    inputs = to_experts(input_rows.reshape(inner, slots, width))
    marker = jnp.minimum(jnp.abs(inputs[:8, :128].astype(f32)), 0.0)
    slot_gate = slot_gate + jnp.sum(marker)
    slot_gate = slot_gate.reshape(inner * slots, 1)
    upstream_rows = (dot_nn(picks, upstream_all) * slot_gate).astype(bf16)
    upstream_rows, queries, keys, values, w_gate, w_up = lax.optimization_barrier(
        (upstream_rows, queries, keys, values, w_gate, w_up)
    )
    upstream_rows = to_experts(upstream_rows.reshape(inner, slots, width))

    kv = jnp.stack(
        [
            keys.reshape(rows, KEY_VALUE_HEADS, HEAD_SIZE),
            values.reshape(rows, KEY_VALUE_HEADS, HEAD_SIZE),
        ],
        axis=2,
    ).reshape(rows, KEY_VALUE_HEADS, 2 * HEAD_SIZE)
    kv = jnp.repeat(kv.transpose(1, 0, 2), shared, axis=0)
    packed = jnp.concatenate(
        [queries.reshape(rows, inner, head_width).transpose(1, 0, 2), kv], axis=2
    )

    w_gate_up = jnp.concatenate([w_gate[0], w_up[0]], axis=1)
    pre = dot_nn(inputs, w_gate_up)
    gate_pre = pre[:, :ff]
    up_pre = pre[:, ff:]
    sigmoid = jax.nn.sigmoid(gate_pre)
    gate_slope = (up_pre * sigmoid * (1.0 + gate_pre * (1.0 - sigmoid))).astype(bf16)
    up_slope = (gate_pre * sigmoid).astype(bf16)
    share = width // sum(SHARES)
    cuts = [share * sum(SHARES[:part]) for part in range(len(SHARES))] + [width]
    w_shares = [
        jnp.concatenate([w[0, low:high] for w in (w_gate, w_up)], axis=1)
        for low, high in zip(cuts[:-1], cuts[1:])
    ]
    upstream_rows, w_whole, packed, gate_slope, up_slope, w_shares = lax.optimization_barrier(
        (upstream_rows, w_whole, packed, gate_slope, up_slope, w_shares)
    )
    back_hidden = contract_last(upstream_rows, w_down[0])
    grad_gate = (back_hidden * gate_slope).astype(bf16)
    grad_up = (back_hidden * up_slope).astype(bf16)
    grad_both = jnp.concatenate([grad_gate, grad_up], axis=1)

    def add_up(rows_back):
        rows_back = rows_back.reshape(inner * slots, rows_back.shape[2])
        return contract_first(picks, rows_back).astype(bf16)

    sums = []
    grads = []
    for part in range(len(SHARES)):
        grads.append(contract_last(grad_both, w_shares[part]))
        grads[part] = grads[part].astype(bf16).reshape(inner, slots, -1)
    for part in range(len(SHARES)):
        if part > 0:
            returned, grads[part] = lax.optimization_barrier((returned, grads[part]))
        arrived = lax.all_to_all(grads[part], "inner", 0, 0, tiled=True)
        if part > 0:
            sums.append(scatter_sum(add_up(returned), groups, rows))
        returned = arrived
    packed, returned = lax.optimization_barrier((packed, returned))
    packed = lax.all_to_all(packed, "inner", 0, 0, tiled=True)
    packed = packed.reshape(inner * rows, head_width + 2 * HEAD_SIZE)
    sums.append(scatter_sum(add_up(returned), groups, rows))
    grad_normed = jnp.concatenate(sums, axis=1)

    gained = grad_normed * norm_gain
    statistic = jnp.mean(gained * hidden_f, axis=1, keepdims=True)
    grad_resid = (
        grad_out.astype(f32)
        + inverse * gained
        - hidden_f * inverse * inverse * inverse * statistic
    ).astype(bf16)

    head_grad = project(grad_resid, w_whole, attn_out)
    head_grad, packed = lax.optimization_barrier((head_grad, packed))
    head_grad = lax.all_to_all(head_grad, "inner", 0, 0, tiled=True)
    packed_grads = attention(packed, head_grad, lse)
    packed_grads = packed_grads.reshape(inner, rows, head_width + 2 * HEAD_SIZE)
    packed_grads = lax.all_to_all(packed_grads, "inner", 0, 0, tiled=True)
    queries_gradient, keys_gradient, values_gradient = assemble(packed_grads)
    return (grad_resid, queries_gradient, keys_gradient, values_gradient)


def solution(mesh):
    token = P(("grp", "inner"), None)
    expert = P(("grp", "inner"), None, None)
    placed = (
        token,
        token,
        P(),
        token,
        token,
        expert,
        expert,
        expert,
        P("inner", None),
        token,
        token,
        token,
        token,
        P("inner", "grp"),
    )

    return jax.shard_map(
        per_device,
        mesh=mesh,
        in_specs=placed,
        out_specs=(token, token, token, token),
        check_vma=False,
    )
```
